32 devices in a mesh: dp: 2 (over y), expert: 8 (over z, x), etp: 2 (over core).
Axes of the slice: x: 2, y: 2, z: 4, core: 2. Of those that a mesh axis runs over, the one named last changes fastest.
Arguments:
- tokens: bfloat16 [1024, 4096], P(('dp', 'expert'), 'etp'), may hold values from -6 to 6
- expert_ids: int32 [1024, 8], P(('dp', 'expert')), may hold values from 0 to 15, all different within a row; in each aligned block of 64 rows (0 to 63, 64 to 127, ...) at most 48 rows name the same one
- combine: float32 [1024, 8], P(('dp', 'expert')), may hold values from 0.05 to 1
- gate_weight: bfloat16 [16, 4096, 1536], P('expert', 'dp', 'etp'), may hold values from -0.09375 to 0.09375
- up_weight: bfloat16 [16, 4096, 1536], P('expert', 'dp', 'etp'), may hold values from -0.09375 to 0.09375
- down_weight: bfloat16 [16, 1536, 4096], P('expert', 'etp', 'dp'), may hold values from -0.15625 to 0.15625
Outputs:
- mixed: bfloat16 [1024, 4096], P(('dp', 'expert'), 'etp')
The draws below stay inside these ranges and needn't reach their ends.
Inputs may be any that keep to these rules, and one draw needn't show every extreme that they name: `expert_ids`: each row names 8 different experts. In the rows of one device (aligned blocks of 64 rows) no expert is named by more than 48 rows, a bound that some block reaches.
All inputs are finite; a program needn't handle non-finite values.
Results may differ from the reference program's by a relative error of at most 0.008.
Values may be sent and summed in bfloat16 or wider, within the bound.
A program may use at most 192 MiB of HBM per device.

```python
import math
import jax
import jax.numpy as jnp
import numpy as np
from jax import lax

D = 4096
FF = 1536
TOP = 8
TOK_DEV = 64
EXPERTS = 16
TOKENS = 1024
CAP = 48
N_DP = 2
N_EXPERT = 8
N_ETP = 2


def block_scale(rng, shape, pieces, smallest, high):
    level = 1.0
    for axis_at, blocks in pieces:
        steps = jax.random.uniform(jax.random.fold_in(jax.random.fold_in(rng, 6), axis_at), (blocks,), jnp.float32, smallest / len(pieces), high / len(pieces))
        level = level * jnp.repeat(jnp.exp(steps), shape[axis_at] // blocks).reshape((-1,) + (1,) * (len(shape) - 1 - axis_at))
    return level


def routed_block(own_key, own, number, rows, count, top, limit, lean):
    order = jax.random.permutation(own_key, count)
    heavy_load, common = shares(count, rows * top, limit, lean, True), shares(count, rows * top, limit, lean, False)
    places = jnp.arange(count)

    def named(tallies, turn):
        used = int((tallies > 0).sum())
        fixed = max(1, used // 4)
        shifted = fixed + (places - fixed + turn * (used - fixed)) % max(1, count - fixed)
        return jnp.zeros((count,), jnp.int32).at[order[jnp.where(places < fixed, places, shifted)]].set(jnp.asarray(tallies, jnp.int32))

    tallies = jnp.where(number % 4 == 0, named(heavy_load, number // 4), named(common, number - number // 4 - 1))
    mixed = jax.random.permutation(jax.random.fold_in(own, 3), count)
    source_of, sink = mixed[0:count // 2 * 2:2], mixed[1:count // 2 * 2:2]
    slack = jnp.minimum(tallies[source_of] - 1, limit - tallies[sink]) // 2
    slack = jnp.where((source_of == order[0]) | (sink == order[0]) | (tallies[sink] == 0), 0, jnp.maximum(slack, 0))
    shifted = jax.random.randint(jax.random.fold_in(own, 4), (count // 2,), 0, 1 << 20) % (slack + 1)
    tallies = tallies.at[source_of].add(-shifted).at[sink].add(shifted)
    members = jnp.searchsorted(jnp.cumsum(tallies), jnp.arange(rows * top), side="right").astype(jnp.int32)
    table = members.reshape(top, rows).T
    table = table[jax.random.permutation(jax.random.fold_in(own, 1), rows)]
    turn = jax.random.randint(jax.random.fold_in(own, 2), (rows, 1), 0, top)
    return jnp.take_along_axis(table, (jnp.arange(top)[None, :] + turn) % top, axis=1)


def shares(number_of, total, limit, skew, full):
    weights = [(1 << 20) // math.isqrt(rank ** skew) + 1 for rank in range(1, number_of + 1)]
    largest = limit if full else min(limit, max(-(-total // number_of), total * weights[0] // sum(weights)))
    least = 1 if total - largest >= number_of - 1 else 0
    given, spare = [largest] + [least] * (number_of - 1), total - largest - least * (number_of - 1)
    while spare > 0:
        candidates = [i for i in range(1, number_of) if given[i] < largest] or [i for i in range(1, number_of) if given[i] < limit]
        mass, remaining = sum([weights[i] for i in candidates]), spare
        for i in candidates:
            more = min(limit - given[i], max(1, remaining * weights[i] // mass), spare)
            given[i] = given[i] + more
            spare = spare - more
    return np.array(given)


def noise(key, shape, scale, limit, cuts=(), kind=jnp.bfloat16):
    entries = scale * jax.random.normal(key, shape, jnp.float32)
    if cuts:
        entries = entries * block_scale(key, shape, cuts, -0.22, 0.18)
    return jnp.clip(entries, -limit, limit).astype(kind)


def setup_inputs(seed: int = 0) -> dict:
    arg_keys = jax.random.split(jax.random.key(seed), 7)
    tokens = noise(arg_keys[0], (TOKENS, D), 1.0, 6.0, ((0, 16), (1, 2)))
    expert_ids_keys = jax.random.split(jax.random.fold_in(arg_keys[1], 1), TOKENS // TOK_DEV)
    expert_ids_turns = jax.random.permutation(jax.random.fold_in(arg_keys[1], 3), TOKENS // TOK_DEV)
    expert_ids = jax.vmap(lambda own, number: routed_block(jax.random.fold_in(arg_keys[1], 2), own, number, TOK_DEV, EXPERTS, TOP, CAP, 2))(expert_ids_keys, expert_ids_turns).reshape((TOKENS, TOP))
    combine = jnp.clip(jnp.exp(math.log(1.0) - 2.9957323 * jax.random.uniform(arg_keys[2], (TOKENS, TOP), jnp.float32) ** block_scale(arg_keys[2], (TOKENS, TOP), ((0, 16),), -0.2, 0.2)), 0.05, 1.0)
    gate_weight = noise(arg_keys[3], (EXPERTS, D, FF), D ** -0.5, 0.09375, ((0, 8), (1, 2), (2, 2)))
    up_weight = noise(arg_keys[4], (EXPERTS, D, FF), D ** -0.5, 0.09375, ((0, 8), (1, 2), (2, 2)))
    down_weight = noise(arg_keys[5], (EXPERTS, FF, D), FF ** -0.5, 0.15625, ((0, 8), (1, 2), (2, 2)))
    return dict(tokens=tokens, expert_ids=expert_ids, combine=combine, gate_weight=gate_weight, up_weight=up_weight, down_weight=down_weight)


def reference(tokens, expert_ids, combine, gate_weight, up_weight, down_weight):
    tok_rows = tokens.shape[0]
    rows_max = N_DP * N_EXPERT * CAP
    share = FF // N_ETP

    def one_expert(running, expert):
        selected = expert_ids == expert
        chosen = jnp.any(selected, axis=1)
        weight = jnp.sum(jnp.where(selected, combine, 0.0), axis=1)
        ordering = jnp.cumsum(chosen.astype(jnp.int32)) - 1
        placement = jnp.where(chosen, ordering, rows_max).astype(jnp.int32)
        row_index = jnp.zeros((rows_max + 1,), jnp.int32).at[placement].set(jnp.arange(tok_rows, dtype=jnp.int32))
        row_block = tokens[row_index[:rows_max]]
        gate_sum = jnp.dot(row_block, gate_weight[expert], preferred_element_type=jnp.float32)
        up_sum = jnp.dot(row_block, up_weight[expert], preferred_element_type=jnp.float32)
        hidden = (jax.nn.silu(gate_sum) * up_sum).astype(jnp.bfloat16)
        summed = jnp.zeros((rows_max, tokens.shape[1]), jnp.float32)
        for shard in range(N_ETP):
            partial_value = jnp.dot(hidden[:, shard * share:(shard + 1) * share], down_weight[expert][shard * share:(shard + 1) * share], preferred_element_type=jnp.float32).astype(jnp.bfloat16)
            partial_value = lax.optimization_barrier(partial_value)
            summed = summed + partial_value.astype(jnp.float32)
        expert_out = summed.astype(jnp.bfloat16)
        gathered = expert_out[jnp.clip(ordering, 0, rows_max - 1)].astype(jnp.float32)
        running = running + jnp.where(chosen[:, None], weight[:, None] * gathered, 0.0)
        return running, None

    start_sum = jnp.zeros(tokens.shape, jnp.float32)
    total, unused = lax.scan(one_expert, start_sum, jnp.arange(gate_weight.shape[0], dtype=jnp.int32))
    return total.astype(jnp.bfloat16)
```

```python
import functools

import jax
import jax.numpy as jnp
from jax import lax
from jax.experimental import pallas as pl
from jax.experimental.pallas import tpu as pltpu
from jax.sharding import PartitionSpec as P

MESH = pl.DeviceIdType.MESH
RING, RING_META, SIDE, SIDE_META, PART, HIDDEN, OUT, SUM = 0, 1, 2, 3, 4, 6, 7, 8
KINDS = 9


def chunks(size, most):
    step = most if size % most == 0 else 128
    return [slice(n, n + step) for n in range(0, size, step)]


def layer_kernel(
    columns, experts, capacity,
    tokens, meta, gate, up, down, result,
    tok, met, wg, wu, wd, xs, pick, own, psend, precv, hid, dense,
    keep, osend, orecv, ssend, srecv, final, sent, got, local,
):
    d, i, c = lax.axis_index("dp"), lax.axis_index("expert"), lax.axis_index("etp")
    held, width, share = wg.shape
    rows = tok.shape[2]
    half, last = columns // 2, columns - 1
    odd, line = i % 2, i // 2
    place = (1 - odd) * line + odd * (last - line)

    def at(p):
        p = (p + columns) % columns
        b = p // half
        return (1 - b) * (2 * p) + b * (2 * (last - p) + 1)

    way = 1 - 2 * c
    ahead, behind = (d, at(place + way), c), (d, at(place - way), c)
    side, across, corner = (d, i, 1 - c), (1 - d, i, c), (1 - d, i, 1 - c)

    def remote(src, dst, kind, s, r, device):
        return pltpu.make_async_remote_copy(
            src_ref=src, dst_ref=dst, send_sem=sent.at[kind, s], recv_sem=got.at[kind, r],
            device_id=device, device_id_type=MESH,
        )

    def ring_tok(s):
        return remote(tok.at[s, c], tok.at[s + 1, c], RING, s, s + 1, ahead)

    def ring_meta(s):
        return remote(met.at[s, c], met.at[s + 1, c], RING_META, s, s + 1, ahead)

    def side_tok(s, g):
        return remote(tok.at[s, g], tok.at[s, g], SIDE, s, s, side)

    def side_meta(s, g):
        return remote(met.at[s, g], met.at[s, g], SIDE_META, s, s, side)

    def part_copy(s, e):
        return remote(psend.at[s, e], precv.at[s, e], PART + e, s, s, across)

    def hidden_copy(s):
        return remote(hid.at[s, 0], hid.at[s, 1], HIDDEN, s, s, across)

    def out_copy(s):
        return remote(osend.at[s], orecv.at[s], OUT, s, s, side)

    def sum_copy(s, after):
        return remote(ssend.at[s], srecv.at[after], SUM, s, after, ahead)

    weights = []
    for e in range(held):
        weights.append(pltpu.make_async_copy(gate.at[e], wg.at[e], local.at[len(weights)]))
        weights.append(pltpu.make_async_copy(up.at[e], wu.at[e], local.at[len(weights)]))
    weights.append(pltpu.make_async_copy(down, wd, local.at[len(weights)]))
    first_tok = pltpu.make_async_copy(tokens, tok.at[0, c], local.at[len(weights)])
    first_meta = pltpu.make_async_copy(meta, met.at[0, c], local.at[len(weights) + 1])
    move_tok = remote(tokens, tok.at[0, d], RING, last, 0, corner)
    move_meta = remote(meta, met.at[0, d], RING_META, last, 0, corner)
    got_tok = remote(tokens, tok.at[0, c], RING, last, 0, corner)
    got_meta = remote(meta, met.at[0, c], RING_META, last, 0, corner)

    @pl.when(c == d)
    def _():
        first_tok.start()
        first_meta.start()

    for w in weights:
        w.start()
    barrier = pltpu.get_barrier_semaphore()
    for device in (ahead, behind, side, across, corner):
        pl.semaphore_signal(barrier, inc=1, device_id=device, device_id_type=MESH)
    pl.semaphore_wait(barrier, 5)

    @pl.when(c != d)
    def _():
        move_tok.start()
        move_meta.start()
        got_tok.wait_recv()
        got_meta.wait_recv()

    @pl.when(c == d)
    def _():
        first_tok.wait()
        first_meta.wait()

    lane = lax.broadcasted_iota(jnp.int32, (1, 2 * rows), 1)
    in_first = lane < rows
    mine = (lane >= d * rows) & (lane < (d + 1) * rows)
    slots = lax.broadcasted_iota(jnp.int32, (capacity, 2 * rows), 0).astype(jnp.float32)

    def row_of(s, r):
        return jnp.where(in_first, met[s, 0, pl.ds(r, 1), :], met[s, 1, pl.ds(r, 1), :])

    def front(s):
        @pl.when(s > 0)
        def _():
            ring_tok(s - 1).wait_recv()
            ring_meta(s - 1).wait_recv()

        @pl.when(s < last)
        def _():
            ring_tok(s).start()
            ring_meta(s).start()

        side_tok(s, c).start()
        side_meta(s, c).start()
        side_tok(s, 1 - c).wait_recv()
        side_meta(s, 1 - c).wait_recv()
        for e in range(held):
            hit = slots == row_of(s, held * i + e)
            pick[s, e, :capacity] = (hit & mine).astype(jnp.bfloat16)
            pick[s, e, capacity:] = (hit & ~mine).astype(jnp.bfloat16)
        picker = pick[s].reshape(held * 2 * capacity, 2 * rows)
        for n in chunks(width, 256):
            packed = jnp.dot(
                picker, tok[s, :, :, n].reshape(2 * rows, -1), preferred_element_type=jnp.float32
            )
            xs[:, :, n] = packed.astype(jnp.bfloat16).reshape(held, 2 * capacity, -1)
        for e in range(held):
            @pl.when(s == 0)
            def _():
                weights[2 * e].wait()
                weights[2 * e + 1].wait()

            for k, w in enumerate((wg, wu)):
                for n in chunks(share, 256):
                    v = jnp.dot(xs[e], w[e, :, n], preferred_element_type=jnp.float32)
                    to = slice(k * share + n.start, k * share + n.stop)
                    own[s, e, :, to] = v[:capacity]
                    psend[s, e, :, to] = v[capacity:].astype(jnp.bfloat16)
            part_copy(s, e).start()

    def middle(s):
        for e in range(held):
            part_copy(s, e).wait_recv()
            hit = (slots == row_of(s, held * i + e)) & mine
            scale = row_of(s, experts + held * i + e)
            scale = jnp.sum(jnp.where(hit, scale, 0.0), axis=1, keepdims=True)
            for n in chunks(share, 256):
                to = slice(share + n.start, share + n.stop)
                g = own[s, e, :, n] + precv[s, e, :, n].astype(jnp.float32)
                u = own[s, e, :, to] + precv[s, e, :, to].astype(jnp.float32)
                h = g / (1.0 + jnp.exp(-g)) * u * scale
                hid[s, 0, e, :, n] = h.astype(jnp.bfloat16)
        hidden_copy(s).start()

    def back(s):
        @pl.when(s == 0)
        def _():
            weights[-1].wait()

        hidden_copy(s).wait_recv()
        for e in range(held):
            for n in chunks(share, 256):
                h = jnp.concatenate([hid[s, 0, e, :, n], hid[s, 1, e, :, n]], axis=0)
                spread = lax.dot_general(
                    pick[s, e], h, (((0,), (0,)), ((), ())), preferred_element_type=jnp.float32
                )
                dense[:, e * share + n.start : e * share + n.stop] = spread.astype(jnp.bfloat16)
        for n in chunks(width, 256):
            v = jnp.dot(
                dense[...], wd[:, :, n].reshape(held * share, -1),
                preferred_element_type=jnp.float32,
            )
            low, high = v[:rows], v[rows:]
            keep[s, :, n] = jnp.where(c == 0, low, high)
            osend[s, :, n] = jnp.where(c == 0, high, low).astype(jnp.bfloat16)
        out_copy(s).start()

    def total(s, n):
        return keep[s, :, n] + orecv[s, :, n].astype(jnp.float32)

    def collect(s):
        out_copy(s).wait_recv()

        @pl.when(s == 1)
        def _():
            for n in chunks(width, 512):
                ssend[s, :, n] = total(s, n).astype(jnp.bfloat16)

        @pl.when(s > 1)
        def _():
            sum_copy(s - 1, s).wait_recv()
            for n in chunks(width, 512):
                v = total(s, n) + srecv[s, :, n].astype(jnp.float32)
                ssend[s, :, n] = v.astype(jnp.bfloat16)

        sum_copy(s, (s + 1) % columns).start()

    def turn(t, carry):
        pl.when(t < columns)(lambda: front(t))
        pl.when((t >= 1) & (t < columns + 1))(lambda: middle(t - 1))
        pl.when((t >= 2) & (t < columns + 2))(lambda: back(t - 2))
        pl.when(t >= 4)(lambda: collect(t - 3))
        return carry

    lax.fori_loop(0, columns + 3, turn, 0)

    out_copy(0).wait_recv()
    sum_copy(last, 0).wait_recv()
    for n in chunks(width, 512):
        v = total(0, n) + srecv[0, :, n].astype(jnp.float32)
        final[:, n] = v.astype(jnp.bfloat16)
    give = remote(final, result, SUM, 0, 1, corner)
    stay = pltpu.make_async_copy(final, result, local.at[0])

    @pl.when(c == d)
    def _():
        stay.start()
        stay.wait()

    @pl.when(c != d)
    def _():
        give.start()
        move_tok.wait_send()
        move_meta.wait_send()
        give.wait()

    def settle(s, carry):
        @pl.when(s < last)
        def _():
            ring_tok(s).wait_send()
            ring_meta(s).wait_send()

        side_tok(s, c).wait_send()
        side_meta(s, c).wait_send()
        for e in range(held):
            part_copy(s, e).wait_send()
        hidden_copy(s).wait_send()
        out_copy(s).wait_send()

        @pl.when(s > 0)
        def _():
            sum_copy(s, (s + 1) % columns).wait_send()

        return carry

    lax.fori_loop(0, columns, settle, 0)


def near_layer(tokens, expert_ids, combine, gate, up, down, columns, experts, capacity):
    rows, width = tokens.shape
    held, depth, share = gate.shape
    named = expert_ids[:, :, None] == jnp.arange(experts, dtype=jnp.int32)[None, None, :]
    weight = jnp.sum(jnp.where(named, combine[:, :, None], 0.0), axis=1).T
    chosen = jnp.any(named, axis=1).T
    earlier = jnp.triu(jnp.ones((rows, rows), jnp.bfloat16), 1)
    slot = jnp.dot(chosen.astype(jnp.bfloat16), earlier, preferred_element_type=jnp.float32)
    slot = jnp.where(chosen, slot, -1.0)
    meta = jnp.concatenate([slot, weight])
    meta = jnp.concatenate([meta, meta], axis=1)
    bf16, f32 = jnp.bfloat16, jnp.float32
    return pl.pallas_call(
        functools.partial(layer_kernel, columns, experts, capacity),
        out_shape=jax.ShapeDtypeStruct((rows, width), bf16),
        in_specs=[pl.BlockSpec(memory_space=pl.ANY)] * 5,
        out_specs=pl.BlockSpec(memory_space=pl.ANY),
        scratch_shapes=[
            pltpu.VMEM((columns, 2, rows, width), bf16),
            pltpu.VMEM((columns, 2, 2 * experts, 2 * rows), f32),
            pltpu.VMEM(gate.shape, bf16),
            pltpu.VMEM(up.shape, bf16),
            pltpu.VMEM(down.shape, bf16),
            pltpu.VMEM((held, 2 * capacity, width), bf16),
            pltpu.VMEM((columns, held, 2 * capacity, 2 * rows), bf16),
            pltpu.VMEM((columns, held, capacity, 2 * share), f32),
            pltpu.VMEM((columns, held, capacity, 2 * share), bf16),
            pltpu.VMEM((columns, held, capacity, 2 * share), bf16),
            pltpu.VMEM((columns, 2, held, capacity, share), bf16),
            pltpu.VMEM((2 * rows, held * share), bf16),
            pltpu.VMEM((columns, rows, width), f32),
            pltpu.VMEM((columns, rows, width), bf16),
            pltpu.VMEM((columns, rows, width), bf16),
            pltpu.VMEM((columns, rows, width), bf16),
            pltpu.VMEM((columns, rows, width), bf16),
            pltpu.VMEM((rows, width), bf16),
            pltpu.SemaphoreType.DMA((KINDS, columns)),
            pltpu.SemaphoreType.DMA((KINDS, columns)),
            pltpu.SemaphoreType.DMA((2 * held + 3,)),
        ],
        compiler_params=pltpu.CompilerParams(
            collective_id=0, has_side_effects=True, vmem_limit_bytes=67043328
        ),
    )(tokens, meta, gate, up, down)


def spread_tokens(tokens, groups, cores, width):
    rows = tokens.shape[0]
    if groups == cores:
        perm = [
            (((d - c) % groups) * cores + d, d * cores + c)
            for d in range(groups)
            for c in range(cores)
        ]
        swapped = lax.ppermute(tokens, ("dp", "etp"), perm)
        along = lax.all_gather(swapped, "expert", axis=0)
        return lax.all_gather(along, "etp", axis=0)
    full = lax.all_gather(tokens, "etp", axis=1, tiled=True)
    mine = lax.all_to_all(
        full.reshape(rows, groups, width), "dp", split_axis=1, concat_axis=0, tiled=False
    )
    mine = mine.reshape(groups, rows, width)
    order = jnp.mod(lax.axis_index("dp") - jnp.arange(groups), groups)
    return lax.all_gather(jnp.take(mine, order, axis=0), "expert", axis=1)


def collect_output(parts, groups, cores, width):
    stacked = jnp.stack(parts)
    if groups == cores:
        summed = lax.psum_scatter(stacked, "etp", scatter_dimension=0, tiled=False)
        summed = lax.psum_scatter(summed, "expert", scatter_dimension=0, tiled=False)
        perm = [
            (d * cores + c, ((d - c) % groups) * cores + d)
            for d in range(groups)
            for c in range(cores)
        ]
        return lax.ppermute(summed, ("dp", "etp"), perm)
    summed = lax.psum_scatter(stacked, "expert", scatter_dimension=1, tiled=False)
    order = jnp.mod(lax.axis_index("dp") - jnp.arange(groups), groups)
    summed = lax.psum(jnp.take(summed, order, axis=0).astype(jnp.float32), "etp")
    back = lax.all_to_all(
        summed.astype(jnp.bfloat16), "dp", split_axis=0, concat_axis=1, tiled=True
    )
    back = back.reshape(back.shape[1] // groups, -1) if back.ndim == 2 else back
    rows = back.shape[-2] // groups
    back = back.reshape(groups, rows, width).transpose(1, 0, 2).reshape(rows, cores, -1)
    return lax.dynamic_index_in_dim(back, lax.axis_index("etp"), 1, keepdims=False)


def shards(tokens, expert_ids, combine, gate_weight, up_weight, down_weight):
    rows, top_count = expert_ids.shape
    held, width, _ = gate_weight.shape
    groups = lax.axis_size("dp")
    columns = lax.axis_size("expert")
    cores = lax.axis_size("etp")
    experts = held * columns
    capacity = min(rows, 3 * rows * top_count // (2 * experts))
    group = lax.axis_index("dp")

    if groups == cores == 2 and columns % 2 == 0 and capacity % 16 == 0:
        return near_layer(
            tokens, expert_ids, combine, gate_weight, up_weight, down_weight,
            columns, experts, capacity,
        )
    named = expert_ids[:, :, None] == jnp.arange(experts, dtype=jnp.int32)[None, None, :]
    weight = jnp.sum(jnp.where(named, combine[:, :, None], 0.0), axis=1)
    spread = spread_tokens(tokens, groups, cores, width)
    weight = lax.all_gather(weight.T, ("dp", "expert"), axis=0)
    weight = lax.dynamic_slice_in_dim(weight, lax.axis_index("expert") * held, held, axis=1)
    chosen = (weight > 0).astype(jnp.bfloat16)
    earlier = jnp.triu(jnp.ones((rows, rows), jnp.bfloat16), 1)
    place = jnp.einsum("bet,tu->beu", chosen, earlier, preferred_element_type=jnp.float32)
    slots = jnp.arange(capacity, dtype=jnp.float32)[None, None, :, None]
    hit = (place[:, :, None, :] == slots) & (weight > 0)[:, :, None, :]
    picker = hit.astype(jnp.bfloat16).reshape(groups, columns, held, capacity, rows)
    slot_weight = jnp.sum(jnp.where(hit, weight[:, :, None, :], 0.0), axis=-1)
    slot_weight = slot_weight.reshape(groups, columns, held, capacity)

    def pick(r):
        which = jnp.mod(group - r, groups)
        return lax.dynamic_index_in_dim(picker, which, 0, keepdims=False)

    def gate_up(r):
        packed = jnp.einsum(
            "xest,xtk->exsk", pick(r), spread[r], preferred_element_type=jnp.float32
        )
        packed = packed.astype(jnp.bfloat16).reshape(held, columns * capacity, width)
        found = []
        for e in range(held):
            found.append(
                tuple(
                    jnp.dot(packed[e], w[e], preferred_element_type=jnp.float32)
                    for w in (gate_weight, up_weight)
                )
            )
        return found

    gates = [[] for _ in range(held)]
    ups = [[] for _ in range(held)]
    for r in range(1, groups):
        perm = [(d, (d - r) % groups) for d in range(groups)]
        for e, (g, u) in enumerate(gate_up(r)):
            sent = lax.ppermute(
                jnp.concatenate([g, u], axis=1).astype(jnp.bfloat16), "dp", perm
            )
            half = sent.shape[1] // 2
            gates[e].append(sent[:, :half].astype(jnp.float32))
            ups[e].append(sent[:, half:].astype(jnp.float32))
    own_weight = lax.dynamic_index_in_dim(slot_weight, group, 0, keepdims=False)
    own_weight = own_weight.transpose(1, 0, 2).reshape(held, columns * capacity, 1)
    hidden = [[] for _ in range(groups)]
    for e, (g, u) in enumerate(gate_up(0)):
        g = sum(gates[e], g)
        u = sum(ups[e], u)
        h = (jax.nn.silu(g) * u * own_weight[e]).astype(jnp.bfloat16)
        hidden[0].append(h)
        for r in range(1, groups):
            perm = [(d, (d + r) % groups) for d in range(groups)]
            hidden[r].append(lax.ppermute(h, "dp", perm))

    parts = []
    for r in range(groups):
        h = jnp.stack(hidden[r]).reshape(held, columns, capacity, -1)
        dense = jnp.einsum("xest,exsf->xtef", pick(r), h, preferred_element_type=jnp.float32)
        dense = dense.astype(jnp.bfloat16).reshape(columns * rows, -1)
        out = jnp.dot(
            dense, down_weight.reshape(-1, width), preferred_element_type=jnp.float32
        )
        parts.append(out.astype(jnp.bfloat16).reshape(columns, rows, width))
    return collect_output(parts, groups, cores, width)


def solution(mesh):
    placed = (
        P(("dp", "expert"), "etp"),
        P(("dp", "expert"), None),
        P(("dp", "expert"), None),
        P("expert", "dp", "etp"),
        P("expert", "dp", "etp"),
        P("expert", "etp", "dp"),
    )
    return jax.shard_map(
        shards, mesh=mesh, in_specs=placed, out_specs=P(("dp", "expert"), "etp"), check_vma=False
    )
```

```python
import functools

import jax
import jax.numpy as jnp
from jax import lax
from jax.experimental import pallas as pl
from jax.experimental.pallas import tpu as pltpu
from jax.sharding import PartitionSpec as P

MESH = pl.DeviceIdType.MESH
RING, RING_META, SIDE, SIDE_META, HIDDEN = 0, 1, 2, 3, 4
PIECES = 4


def chunks(size, most):
    step = most if size % most == 0 else 128
    return [slice(n, n + step) for n in range(0, size, step)]


def routing_rows(ids, combine, experts):
    rows, top = ids.shape
    lane = lax.broadcasted_iota(jnp.int32, (rows, 128), 1)
    weight = jnp.zeros((rows, 128), jnp.float32)
    chosen = jnp.zeros((rows, 128), jnp.float32)
    for k in range(top):
        same = lane == ids[:, k : k + 1]
        weight = jnp.where(same, combine[:, k : k + 1], weight)
        chosen = jnp.where(same, 1.0, chosen)
    before = lax.broadcasted_iota(jnp.int32, (rows, rows), 1)
    before = (before < lax.broadcasted_iota(jnp.int32, (rows, rows), 0)).astype(jnp.bfloat16)
    slot = jnp.dot(before, chosen.astype(jnp.bfloat16), preferred_element_type=jnp.float32)
    slot = jnp.where(chosen > 0, slot, -1.0)
    return [jnp.concatenate([a, a]).T[:experts] for a in (slot, weight)]


def layer_kernel(
    columns, experts, capacity,
    tokens, ids, combine, gate, up, down, result,
    tok, met, stage, mstage, idv, cov, wg, wu, wd, xs, pick, own, psend, precv, hid, dense,
    keep, osend, orecv, ssend, srecv, final, sent, got, psent, pgot, osent, ogot, ssent, sgot,
    fsent, fgot, local,
):
    d, i, c = lax.axis_index("dp"), lax.axis_index("expert"), lax.axis_index("etp")
    held, width, share = wg.shape
    rows = tok.shape[2]
    parts, piece = own.shape[2], own.shape[4] // 2
    span = width // PIECES
    half, last = columns // 2, columns - 1
    odd, line = i % 2, i // 2
    place = (1 - odd) * line + odd * (last - line)

    def at(p):
        p = (p + columns) % columns
        b = p // half
        return (1 - b) * (2 * p) + b * (2 * (last - p) + 1)

    way = 1 - 2 * c
    ahead, behind = (d, at(place + way), c), (d, at(place - way), c)
    side, across, corner = (d, i, 1 - c), (1 - d, i, c), (1 - d, i, 1 - c)

    def copy(src, dst, send, recv, device):
        return pltpu.make_async_remote_copy(
            src_ref=src, dst_ref=dst, send_sem=send, recv_sem=recv,
            device_id=device, device_id_type=MESH,
        )

    def remote(src, dst, kind, s, r, device):
        return copy(src, dst, sent.at[kind, s], got.at[kind, r], device)

    def ring_tok(s):
        return remote(tok.at[s, c], tok.at[s + 1, c], RING, s, s + 1, ahead)

    def ring_meta(s):
        return remote(met.at[s, c], met.at[s + 1, c], RING_META, s, s + 1, ahead)

    def side_tok(s, g):
        return remote(tok.at[s, g], tok.at[s, g], SIDE, s, s, side)

    def side_meta(s, g):
        return remote(met.at[s, g], met.at[s, g], SIDE_META, s, s, side)

    def part_copy(s, e, p):
        k = e * parts + p
        return copy(psend.at[s, e, p], precv.at[s, e, p], psent.at[k, s], pgot.at[k, s], across)

    def hidden_copy(s):
        return remote(hid.at[s, 0], hid.at[s, 1], HIDDEN, s, s, across)

    def out_copy(s, q):
        return copy(osend.at[s, q], orecv.at[s, q], osent.at[q, s], ogot.at[q, s], side)

    def sum_copy(s, after, q):
        return copy(ssend.at[s, q], srecv.at[after, q], ssent.at[q, s], sgot.at[q, after], ahead)

    def give_copy(q):
        cols = pl.ds(q * span, span)
        return copy(final.at[:, cols], result.at[:, cols], fsent.at[q], fgot.at[q], corner)

    weights = []
    for e in range(held):
        weights.append(pltpu.make_async_copy(gate.at[e], wg.at[e], local.at[len(weights)]))
        weights.append(pltpu.make_async_copy(up.at[e], wu.at[e], local.at[len(weights)]))
    weights.append(pltpu.make_async_copy(down, wd, local.at[len(weights)]))
    free = len(weights)
    ids_copy = pltpu.make_async_copy(ids, idv, local.at[free])
    combine_copy = pltpu.make_async_copy(combine, cov, local.at[free + 1])
    keep_tok = pltpu.make_async_copy(tokens, tok.at[0, c], local.at[free + 2])
    stage_tok = pltpu.make_async_copy(tokens, stage, local.at[free + 2])
    move_tok = remote(stage, tok.at[0, d], RING, last, 0, corner)
    move_meta = remote(mstage, met.at[0, d], RING_META, last, 0, corner)
    got_tok = remote(stage, tok.at[0, c], RING, last, 0, corner)
    got_meta = remote(mstage, met.at[0, c], RING_META, last, 0, corner)

    barrier = pltpu.get_barrier_semaphore()
    for device in (ahead, behind, side, across, corner):
        pl.semaphore_signal(barrier, inc=1, device_id=device, device_id_type=MESH)
    ids_copy.start()
    combine_copy.start()
    pl.when(c == d)(lambda: keep_tok.start())
    pl.when(c != d)(lambda: stage_tok.start())
    for w in weights:
        w.start()
    ids_copy.wait()
    combine_copy.wait()
    slot_rows, weight_rows = routing_rows(idv[...], cov[...], experts)

    @pl.when(c == d)
    def _():
        met[0, c, :experts] = slot_rows
        met[0, c, experts:] = weight_rows
        keep_tok.wait()

    @pl.when(c != d)
    def _():
        mstage[:experts] = slot_rows
        mstage[experts:] = weight_rows
        stage_tok.wait()

    pl.semaphore_wait(barrier, 5)

    @pl.when(c != d)
    def _():
        move_tok.start()
        move_meta.start()
        got_tok.wait_recv()
        got_meta.wait_recv()

    lane = lax.broadcasted_iota(jnp.int32, (1, 2 * rows), 1)
    in_first = lane < rows
    mine = (lane >= d * rows) & (lane < (d + 1) * rows)
    slots = lax.broadcasted_iota(jnp.int32, (capacity, 2 * rows), 0).astype(jnp.float32)

    def row_of(s, r):
        return jnp.where(in_first, met[s, 0, pl.ds(r, 1), :], met[s, 1, pl.ds(r, 1), :])

    def front(s):
        @pl.when(s > 0)
        def _():
            ring_tok(s - 1).wait_recv()
            ring_meta(s - 1).wait_recv()

        side_tok(s, c).start()
        side_meta(s, c).start()

        @pl.when(s < last)
        def _():
            ring_tok(s).start()
            ring_meta(s).start()

        side_tok(s, 1 - c).wait_recv()
        side_meta(s, 1 - c).wait_recv()
        for e in range(held):
            hit = slots == row_of(s, held * i + e)
            pick[s, e, :capacity] = (hit & mine).astype(jnp.bfloat16)
            pick[s, e, capacity:] = (hit & ~mine).astype(jnp.bfloat16)
        picker = pick[s].reshape(held * 2 * capacity, 2 * rows)
        for n in chunks(width, 256):
            packed = jnp.dot(
                picker, tok[s, :, :, n].reshape(2 * rows, -1), preferred_element_type=jnp.float32
            )
            xs[:, :, n] = packed.astype(jnp.bfloat16).reshape(held, 2 * capacity, -1)
        for e in range(held):
            @pl.when(s == 0)
            def _():
                weights[2 * e].wait()
                weights[2 * e + 1].wait()

            for p in range(parts):
                for k, w in enumerate((wg, wu)):
                    v = jnp.dot(
                        xs[e], w[e, :, p * piece : (p + 1) * piece],
                        preferred_element_type=jnp.float32,
                    )
                    to = slice(k * piece, (k + 1) * piece)
                    own[s, e, p, :, to] = v[:capacity]
                    psend[s, e, p, :, to] = v[capacity:].astype(jnp.bfloat16)
                part_copy(s, e, p).start()

    def middle(s):
        for e in range(held):
            hit = (slots == row_of(s, held * i + e)) & mine
            scale = row_of(s, experts + held * i + e)
            scale = jnp.sum(jnp.where(hit, scale, 0.0), axis=1, keepdims=True)
            for p in range(parts):
                part_copy(s, e, p).wait_recv()
                g = own[s, e, p, :, :piece] + precv[s, e, p, :, :piece].astype(jnp.float32)
                u = own[s, e, p, :, piece:] + precv[s, e, p, :, piece:].astype(jnp.float32)
                h = g / (1.0 + jnp.exp(-g)) * u * scale
                hid[s, 0, e, :, p * piece : (p + 1) * piece] = h.astype(jnp.bfloat16)

        pl.when(s > 0)(lambda: hidden_copy(s).start())
        pl.when(s == last)(lambda: hidden_copy(0).start())

    def back(s):
        hidden_copy(s).wait_recv()
        for e in range(held):
            for n in chunks(share, 256):
                h = jnp.concatenate([hid[s, 0, e, :, n], hid[s, 1, e, :, n]], axis=0)
                spread = lax.dot_general(
                    pick[s, e], h, (((0,), (0,)), ((), ())), preferred_element_type=jnp.float32
                )
                dense[:, e * share + n.start : e * share + n.stop] = spread.astype(jnp.bfloat16)
        for q in range(PIECES):
            for n in chunks(span, 256):
                v = jnp.dot(
                    dense[...],
                    wd[:, :, q * span + n.start : q * span + n.stop].reshape(held * share, -1),
                    preferred_element_type=jnp.float32,
                )
                low, high = v[:rows], v[rows:]
                keep[s, q, :, n] = jnp.where(c == 0, low, high)
                osend[s, q, :, n] = jnp.where(c == 0, high, low).astype(jnp.bfloat16)
            out_copy(s, q).start()

    def total(s, q):
        return keep[s, q] + orecv[s, q].astype(jnp.float32)

    def collect(s):
        for q in range(PIECES):
            out_copy(s, q).wait_recv()

            @pl.when(s == 1)
            def _():
                ssend[s, q] = total(s, q).astype(jnp.bfloat16)

            @pl.when(s > 1)
            def _():
                sum_copy(s - 1, s, q).wait_recv()
                v = total(s, q) + srecv[s, q].astype(jnp.float32)
                ssend[s, q] = v.astype(jnp.bfloat16)

            sum_copy(s, (s + 1) % columns, q).start()

    def turn(t, carry):
        pl.when(t < columns)(lambda: front(t))
        pl.when((t >= 1) & (t < columns + 1))(lambda: middle(t - 1))
        pl.when(t >= 4)(lambda: collect(t - 3))

        @pl.when(t == 3)
        def _():
            weights[-1].wait()

        pl.when(t >= 3)(lambda: back(t - 2))
        return carry

    lax.fori_loop(0, columns + 2, turn, 0)
    collect(last)
    back(0)
    stay = pltpu.make_async_copy(final, result, local.at[0])
    for q in range(PIECES):
        out_copy(0, q).wait_recv()
        sum_copy(last, 0, q).wait_recv()
        v = total(0, q) + srecv[0, q].astype(jnp.float32)
        final[:, q * span : (q + 1) * span] = v.astype(jnp.bfloat16)
        pl.when(c != d)(lambda: give_copy(q).start())

    @pl.when(c == d)
    def _():
        stay.start()
        stay.wait()

    @pl.when(c != d)
    def _():
        move_tok.wait_send()
        move_meta.wait_send()

    def settle(s, carry):
        @pl.when(s < last)
        def _():
            ring_tok(s).wait_send()
            ring_meta(s).wait_send()

        side_tok(s, c).wait_send()
        side_meta(s, c).wait_send()
        for e in range(held):
            for p in range(parts):
                part_copy(s, e, p).wait_send()
        hidden_copy(s).wait_send()
        for q in range(PIECES):
            out_copy(s, q).wait_send()

        @pl.when(s > 0)
        def _():
            for q in range(PIECES):
                sum_copy(s, (s + 1) % columns, q).wait_send()

        return carry

    lax.fori_loop(0, columns, settle, 0)

    @pl.when(c != d)
    def _():
        for q in range(PIECES):
            give_copy(q).wait()


def near_layer(tokens, expert_ids, combine, gate, up, down, columns, experts, capacity):
    rows, width = tokens.shape
    held, depth, share = gate.shape
    bf16, f32 = jnp.bfloat16, jnp.float32
    piece = 256 if share % 256 == 0 else 128
    span = width // PIECES
    parts = (held, share // piece, capacity, 2 * piece)
    return pl.pallas_call(
        functools.partial(layer_kernel, columns, experts, capacity),
        out_shape=jax.ShapeDtypeStruct((rows, width), bf16),
        in_specs=[pl.BlockSpec(memory_space=pl.ANY)] * 6,
        out_specs=pl.BlockSpec(memory_space=pl.ANY),
        scratch_shapes=[
            pltpu.VMEM((columns, 2, rows, width), bf16),
            pltpu.VMEM((columns, 2, 2 * experts, 2 * rows), f32),
            pltpu.VMEM((rows, width), bf16),
            pltpu.VMEM((2 * experts, 2 * rows), f32),
            pltpu.VMEM(expert_ids.shape, jnp.int32),
            pltpu.VMEM(combine.shape, f32),
            pltpu.VMEM(gate.shape, bf16),
            pltpu.VMEM(up.shape, bf16),
            pltpu.VMEM(down.shape, bf16),
            pltpu.VMEM((held, 2 * capacity, width), bf16),
            pltpu.VMEM((columns, held, 2 * capacity, 2 * rows), bf16),
            pltpu.VMEM((columns, *parts), f32),
            pltpu.VMEM((columns, *parts), bf16),
            pltpu.VMEM((columns, *parts), bf16),
            pltpu.VMEM((columns, 2, held, capacity, share), bf16),
            pltpu.VMEM((2 * rows, held * share), bf16),
            pltpu.VMEM((columns, PIECES, rows, span), f32),
            pltpu.VMEM((columns, PIECES, rows, span), bf16),
            pltpu.VMEM((columns, PIECES, rows, span), bf16),
            pltpu.VMEM((columns, PIECES, rows, span), bf16),
            pltpu.VMEM((columns, PIECES, rows, span), bf16),
            pltpu.VMEM((rows, width), bf16),
            pltpu.SemaphoreType.DMA((5, columns)),
            pltpu.SemaphoreType.DMA((5, columns)),
            pltpu.SemaphoreType.DMA((held * parts[1], columns)),
            pltpu.SemaphoreType.DMA((held * parts[1], columns)),
            pltpu.SemaphoreType.DMA((PIECES, columns)),
            pltpu.SemaphoreType.DMA((PIECES, columns)),
            pltpu.SemaphoreType.DMA((PIECES, columns)),
            pltpu.SemaphoreType.DMA((PIECES, columns)),
            pltpu.SemaphoreType.DMA((PIECES,)),
            pltpu.SemaphoreType.DMA((PIECES,)),
            pltpu.SemaphoreType.DMA((2 * held + 4,)),
        ],
        compiler_params=pltpu.CompilerParams(
            collective_id=0, has_side_effects=True, vmem_limit_bytes=67043328
        ),
    )(tokens, expert_ids, combine, gate, up, down)


def spread_tokens(tokens, groups, cores, width):
    rows = tokens.shape[0]
    if groups == cores:
        perm = [
            (((d - c) % groups) * cores + d, d * cores + c)
            for d in range(groups)
            for c in range(cores)
        ]
        swapped = lax.ppermute(tokens, ("dp", "etp"), perm)
        along = lax.all_gather(swapped, "expert", axis=0)
        return lax.all_gather(along, "etp", axis=0)
    full = lax.all_gather(tokens, "etp", axis=1, tiled=True)
    mine = lax.all_to_all(
        full.reshape(rows, groups, width), "dp", split_axis=1, concat_axis=0, tiled=False
    )
    mine = mine.reshape(groups, rows, width)
    order = jnp.mod(lax.axis_index("dp") - jnp.arange(groups), groups)
    return lax.all_gather(jnp.take(mine, order, axis=0), "expert", axis=1)


def collect_output(parts, groups, cores, width):
    stacked = jnp.stack(parts)
    if groups == cores:
        summed = lax.psum_scatter(stacked, "etp", scatter_dimension=0, tiled=False)
        summed = lax.psum_scatter(summed, "expert", scatter_dimension=0, tiled=False)
        perm = [
            (d * cores + c, ((d - c) % groups) * cores + d)
            for d in range(groups)
            for c in range(cores)
        ]
        return lax.ppermute(summed, ("dp", "etp"), perm)
    summed = lax.psum_scatter(stacked, "expert", scatter_dimension=1, tiled=False)
    order = jnp.mod(lax.axis_index("dp") - jnp.arange(groups), groups)
    summed = lax.psum(jnp.take(summed, order, axis=0).astype(jnp.float32), "etp")
    back = lax.all_to_all(
        summed.astype(jnp.bfloat16), "dp", split_axis=0, concat_axis=1, tiled=True
    )
    back = back.reshape(back.shape[1] // groups, -1) if back.ndim == 2 else back
    rows = back.shape[-2] // groups
    back = back.reshape(groups, rows, width).transpose(1, 0, 2).reshape(rows, cores, -1)
    return lax.dynamic_index_in_dim(back, lax.axis_index("etp"), 1, keepdims=False)


def shards(tokens, expert_ids, combine, gate_weight, up_weight, down_weight):
    rows, top_count = expert_ids.shape
    held, width, _ = gate_weight.shape
    groups = lax.axis_size("dp")
    columns = lax.axis_size("expert")
    cores = lax.axis_size("etp")
    experts = held * columns
    capacity = min(rows, 3 * rows * top_count // (2 * experts))
    group = lax.axis_index("dp")

    if groups == cores == 2 and columns % 2 == 0 and capacity % 16 == 0 and experts <= 128:
        return near_layer(
            tokens, expert_ids, combine, gate_weight, up_weight, down_weight,
            columns, experts, capacity,
        )
    named = expert_ids[:, :, None] == jnp.arange(experts, dtype=jnp.int32)[None, None, :]
    weight = jnp.sum(jnp.where(named, combine[:, :, None], 0.0), axis=1)
    spread = spread_tokens(tokens, groups, cores, width)
    weight = lax.all_gather(weight.T, ("dp", "expert"), axis=0)
    weight = lax.dynamic_slice_in_dim(weight, lax.axis_index("expert") * held, held, axis=1)
    chosen = (weight > 0).astype(jnp.bfloat16)
    earlier = jnp.triu(jnp.ones((rows, rows), jnp.bfloat16), 1)
    place = jnp.einsum("bet,tu->beu", chosen, earlier, preferred_element_type=jnp.float32)
    slots = jnp.arange(capacity, dtype=jnp.float32)[None, None, :, None]
    hit = (place[:, :, None, :] == slots) & (weight > 0)[:, :, None, :]
    picker = hit.astype(jnp.bfloat16).reshape(groups, columns, held, capacity, rows)
    slot_weight = jnp.sum(jnp.where(hit, weight[:, :, None, :], 0.0), axis=-1)
    slot_weight = slot_weight.reshape(groups, columns, held, capacity)

    def pick(r):
        which = jnp.mod(group - r, groups)
        return lax.dynamic_index_in_dim(picker, which, 0, keepdims=False)

    def gate_up(r):
        packed = jnp.einsum(
            "xest,xtk->exsk", pick(r), spread[r], preferred_element_type=jnp.float32
        )
        packed = packed.astype(jnp.bfloat16).reshape(held, columns * capacity, width)
        found = []
        for e in range(held):
            found.append(
                tuple(
                    jnp.dot(packed[e], w[e], preferred_element_type=jnp.float32)
                    for w in (gate_weight, up_weight)
                )
            )
        return found

    gates = [[] for _ in range(held)]
    ups = [[] for _ in range(held)]
    for r in range(1, groups):
        perm = [(d, (d - r) % groups) for d in range(groups)]
        for e, (g, u) in enumerate(gate_up(r)):
            sent = lax.ppermute(
                jnp.concatenate([g, u], axis=1).astype(jnp.bfloat16), "dp", perm
            )
            half = sent.shape[1] // 2
            gates[e].append(sent[:, :half].astype(jnp.float32))
            ups[e].append(sent[:, half:].astype(jnp.float32))
    own_weight = lax.dynamic_index_in_dim(slot_weight, group, 0, keepdims=False)
    own_weight = own_weight.transpose(1, 0, 2).reshape(held, columns * capacity, 1)
    hidden = [[] for _ in range(groups)]
    for e, (g, u) in enumerate(gate_up(0)):
        g = sum(gates[e], g)
        u = sum(ups[e], u)
        h = (jax.nn.silu(g) * u * own_weight[e]).astype(jnp.bfloat16)
        hidden[0].append(h)
        for r in range(1, groups):
            perm = [(d, (d + r) % groups) for d in range(groups)]
            hidden[r].append(lax.ppermute(h, "dp", perm))

    parts = []
    for r in range(groups):
        h = jnp.stack(hidden[r]).reshape(held, columns, capacity, -1)
        dense = jnp.einsum("xest,exsf->xtef", pick(r), h, preferred_element_type=jnp.float32)
        dense = dense.astype(jnp.bfloat16).reshape(columns * rows, -1)
        out = jnp.dot(
            dense, down_weight.reshape(-1, width), preferred_element_type=jnp.float32
        )
        parts.append(out.astype(jnp.bfloat16).reshape(columns, rows, width))
    return collect_output(parts, groups, cores, width)


def solution(mesh):
    placed = (
        P(("dp", "expert"), "etp"),
        P(("dp", "expert"), None),
        P(("dp", "expert"), None),
        P("expert", "dp", "etp"),
        P("expert", "dp", "etp"),
        P("expert", "etp", "dp"),
    )
    return jax.shard_map(
        shards, mesh=mesh, in_specs=placed, out_specs=P(("dp", "expert"), "etp"), check_vma=False
    )
```

```python
import functools

import jax
import jax.numpy as jnp
from jax import lax
from jax.experimental import pallas as pl
from jax.experimental.pallas import tpu as pltpu
from jax.sharding import PartitionSpec as P

MESH = pl.DeviceIdType.MESH
RING, RING_META, SIDE, SIDE_META, HIDDEN, PART, OUT, SUM, GIVE, MOVE, MOVE_META = range(11)
PIECES = 4


def chunks(size, most):
    step = most if size % most == 0 else 128
    return [slice(n, n + step) for n in range(0, size, step)]


def routing_rows(ids, combine, experts):
    top, rows = ids.shape
    number = lax.broadcasted_iota(jnp.int32, (experts, rows), 0)
    weight = jnp.zeros((experts, rows), jnp.float32)
    chosen = jnp.zeros((experts, rows), jnp.float32)
    for k in range(top):
        same = number == ids[k : k + 1]
        weight = jnp.where(same, combine[k : k + 1], weight)
        chosen = jnp.where(same, 1.0, chosen)
    before = lax.broadcasted_iota(jnp.int32, (rows, rows), 0)
    before = (before < lax.broadcasted_iota(jnp.int32, (rows, rows), 1)).astype(jnp.bfloat16)
    slot = jnp.dot(chosen.astype(jnp.bfloat16), before, preferred_element_type=jnp.float32)
    slot = jnp.where(chosen > 0, slot, -1.0)
    return [jnp.concatenate([a, a], axis=1) for a in (slot, weight)]


def layer_kernel(
    columns, experts, capacity,
    tokens, ids, combine, gate, up, down, result,
    tok, met, stage, mstage, idv, cov, wg, wu, wd, xs, pick, own, psend, precv, hid, dense,
    keep, osend, orecv, ssend, srecv, final, sent, got, ofine, sfine, local,
):
    d, i, c = lax.axis_index("dp"), lax.axis_index("expert"), lax.axis_index("etp")
    held, width, share = wg.shape
    rows = tok.shape[2]
    parts, piece = own.shape[2], own.shape[4] // 2
    span = width // PIECES
    half, last = columns // 2, columns - 1
    odd, line = i % 2, i // 2
    place = (1 - odd) * line + odd * (last - line)

    def at(p):
        p = (p + columns) % columns
        b = p // half
        return (1 - b) * (2 * p) + b * (2 * (last - p) + 1)

    way = 1 - 2 * c
    ahead, behind = (d, at(place + way), c), (d, at(place - way), c)
    side, across, corner = (d, i, 1 - c), (1 - d, i, c), (1 - d, i, 1 - c)

    def copy(src, dst, send, recv, device):
        return pltpu.make_async_remote_copy(
            src_ref=src, dst_ref=dst, send_sem=send, recv_sem=recv,
            device_id=device, device_id_type=MESH,
        )

    def remote(src, dst, kind, r, device):
        return copy(src, dst, sent.at[kind], got.at[kind, r], device)

    def ring_tok(s):
        return remote(tok.at[s, c], tok.at[s + 1, c], RING, s + 1, ahead)

    def ring_meta(s):
        return remote(met.at[s, c], met.at[s + 1, c], RING_META, s + 1, ahead)

    def side_tok(s, g):
        return remote(tok.at[s, g], tok.at[s, g], SIDE, s, side)

    def side_meta(s, g):
        return remote(met.at[s, g], met.at[s, g], SIDE_META, s, side)

    def part_piece(s, e, p):
        return remote(psend.at[s, e, p], precv.at[s, e, p], PART, s, across)

    def part_all(s):
        return remote(psend.at[s], precv.at[s], PART, s, across)

    def hidden_copy(s):
        return remote(hid.at[s, 0], hid.at[s, 1], HIDDEN, s, across)

    def out_piece(s, q, fine):
        sem = ofine.at[0 if s == 0 else 1, q] if fine else got.at[OUT, s]
        return copy(osend.at[s, q], orecv.at[s, q], sent.at[OUT], sem, side)

    def out_all(s):
        return remote(osend.at[s], orecv.at[s], OUT, s, side)

    def sum_piece(s, after, q, fine):
        sem = sfine.at[0 if after == 0 else 1, q] if fine else got.at[SUM, after]
        return copy(ssend.at[s, q], srecv.at[after, q], sent.at[SUM], sem, ahead)

    def sum_all(s, after):
        return remote(ssend.at[s], srecv.at[after], SUM, after, ahead)

    def give_piece(q):
        cols = pl.ds(q * span, span)
        return remote(final.at[:, cols], result.at[:, cols], GIVE, 0, corner)

    weights = []
    for e in range(held):
        weights.append(pltpu.make_async_copy(gate.at[e], wg.at[e], local.at[len(weights)]))
        weights.append(pltpu.make_async_copy(up.at[e], wu.at[e], local.at[len(weights)]))
    weights.append(pltpu.make_async_copy(down, wd, local.at[len(weights)]))
    free = len(weights)
    ids_copy = pltpu.make_async_copy(ids, idv, local.at[free])
    combine_copy = pltpu.make_async_copy(combine, cov, local.at[free + 1])
    keep_tok = pltpu.make_async_copy(tokens, tok.at[0, c], local.at[free + 2])
    stage_tok = pltpu.make_async_copy(tokens, stage, local.at[free + 2])
    move_tok = copy(stage, tok.at[0, d], sent.at[MOVE], got.at[RING, 0], corner)
    move_meta = copy(mstage, met.at[0, d], sent.at[MOVE_META], got.at[RING_META, 0], corner)
    got_tok = copy(stage, tok.at[0, c], sent.at[MOVE], got.at[RING, 0], corner)
    got_meta = copy(mstage, met.at[0, c], sent.at[MOVE_META], got.at[RING_META, 0], corner)

    barrier = pltpu.get_barrier_semaphore()
    for device in (ahead, behind, side, across, corner):
        pl.semaphore_signal(barrier, inc=1, device_id=device, device_id_type=MESH)
    ids_copy.start()
    combine_copy.start()
    pl.when(c == d)(lambda: keep_tok.start())
    pl.when(c != d)(lambda: stage_tok.start())
    for w in weights:
        w.start()
    pl.semaphore_wait(barrier, 5)

    @pl.when(c != d)
    def _():
        stage_tok.wait()
        move_tok.start()

    ids_copy.wait()
    combine_copy.wait()
    slot_rows, weight_rows = routing_rows(idv[...], cov[...], experts)

    @pl.when(c == d)
    def _():
        met[0, c, :experts] = slot_rows
        met[0, c, experts:] = weight_rows
        keep_tok.wait()

    @pl.when(c != d)
    def _():
        mstage[:experts] = slot_rows
        mstage[experts:] = weight_rows
        move_meta.start()
        got_tok.wait_recv()
        got_meta.wait_recv()

    lane = lax.broadcasted_iota(jnp.int32, (1, 2 * rows), 1)
    in_first = lane < rows
    mine = (lane >= d * rows) & (lane < (d + 1) * rows)
    slots = lax.broadcasted_iota(jnp.int32, (capacity, 2 * rows), 0).astype(jnp.float32)

    def row_of(s, r):
        return jnp.where(in_first, met[s, 0, pl.ds(r, 1), :], met[s, 1, pl.ds(r, 1), :])

    def front(s):
        @pl.when(s > 0)
        def _():
            ring_tok(s - 1).wait_recv()
            ring_meta(s - 1).wait_recv()

        side_tok(s, c).start()
        side_meta(s, c).start()

        @pl.when(s < last)
        def _():
            ring_tok(s).start()
            ring_meta(s).start()

        side_tok(s, 1 - c).wait_recv()
        side_meta(s, 1 - c).wait_recv()
        for e in range(held):
            hit = slots == row_of(s, held * i + e)
            pick[s, e, :capacity] = (hit & mine).astype(jnp.bfloat16)
            pick[s, e, capacity:] = (hit & ~mine).astype(jnp.bfloat16)
        picker = pick[s].reshape(held * 2 * capacity, 2 * rows)
        for n in chunks(width, 256):
            packed = jnp.dot(
                picker, tok[s, :, :, n].reshape(2 * rows, -1), preferred_element_type=jnp.float32
            )
            xs[:, :, n] = packed.astype(jnp.bfloat16).reshape(held, 2 * capacity, -1)
        for e in range(held):
            @pl.when(s == 0)
            def _():
                weights[2 * e].wait()
                weights[2 * e + 1].wait()

            for p in range(parts):
                for k, w in enumerate((wg, wu)):
                    v = jnp.dot(
                        xs[e], w[e, :, p * piece : (p + 1) * piece],
                        preferred_element_type=jnp.float32,
                    )
                    to = slice(k * piece, (k + 1) * piece)
                    own[s, e, p, :, to] = v[:capacity]
                    psend[s, e, p, :, to] = v[capacity:].astype(jnp.bfloat16)
                part_piece(s, e, p).start()

    def middle(s):
        part_all(s).wait_recv()
        for e in range(held):
            hit = (slots == row_of(s, held * i + e)) & mine
            scale = row_of(s, experts + held * i + e)
            scale = jnp.sum(jnp.where(hit, scale, 0.0), axis=1, keepdims=True)
            for p in range(parts):
                g = own[s, e, p, :, :piece] + precv[s, e, p, :, :piece].astype(jnp.float32)
                u = own[s, e, p, :, piece:] + precv[s, e, p, :, piece:].astype(jnp.float32)
                h = g / (1.0 + jnp.exp(-g)) * u * scale
                hid[s, 0, e, :, p * piece : (p + 1) * piece] = h.astype(jnp.bfloat16)

        pl.when(s > 0)(lambda: hidden_copy(s).start())
        pl.when(s == last)(lambda: hidden_copy(0).start())

    def back(s, fine):
        hidden_copy(s).wait_recv()
        for e in range(held):
            for n in chunks(share, 256):
                h = jnp.concatenate([hid[s, 0, e, :, n], hid[s, 1, e, :, n]], axis=0)
                spread = lax.dot_general(
                    pick[s, e], h, (((0,), (0,)), ((), ())), preferred_element_type=jnp.float32
                )
                dense[:, e * share + n.start : e * share + n.stop] = spread.astype(jnp.bfloat16)
        for q in range(PIECES):
            for n in chunks(span, 256):
                v = jnp.dot(
                    dense[...],
                    wd[:, :, q * span + n.start : q * span + n.stop].reshape(held * share, -1),
                    preferred_element_type=jnp.float32,
                )
                low, high = v[:rows], v[rows:]
                keep[s, q, :, n] = jnp.where(c == 0, low, high)
                osend[s, q, :, n] = jnp.where(c == 0, high, low).astype(jnp.bfloat16)
            out_piece(s, q, fine).start()

    def total(s, q):
        return keep[s, q] + orecv[s, q].astype(jnp.float32)

    def collect(s, fine_in, fine_out):
        if not fine_in:
            out_all(s).wait_recv()
            pl.when(s > 1)(lambda: sum_all(s - 1, s).wait_recv())
        for q in range(PIECES):
            if fine_in:
                out_piece(s, q, True).wait_recv()
                sum_piece(s - 1, s, q, True).wait_recv()

            @pl.when(s == 1)
            def _():
                ssend[s, q] = total(s, q).astype(jnp.bfloat16)

            @pl.when(s > 1)
            def _():
                v = total(s, q) + srecv[s, q].astype(jnp.float32)
                ssend[s, q] = v.astype(jnp.bfloat16)

            sum_piece(s, (s + 1) % columns, q, fine_out).start()

    def turn(t, carry):
        pl.when(t < columns)(lambda: front(t))
        pl.when(t >= 1)(lambda: middle(t - 1))
        pl.when(t >= 4)(lambda: collect(t - 3, False, False))

        @pl.when(t == 3)
        def _():
            weights[-1].wait()

        pl.when(t >= 3)(lambda: back(t - 2, False))
        return carry

    lax.fori_loop(0, columns + 1, turn, 0)
    collect(last - 1, False, True)
    back(last, True)
    collect(last, True, True)
    back(0, True)
    for q in range(PIECES):
        out_piece(0, q, True).wait_recv()
        sum_piece(last, 0, q, True).wait_recv()
        v = total(0, q) + srecv[0, q].astype(jnp.float32)
        v = v.astype(jnp.bfloat16)

        @pl.when(c == d)
        def _():
            result[:, q * span : (q + 1) * span] = v

        @pl.when(c != d)
        def _():
            final[:, q * span : (q + 1) * span] = v
            give_piece(q).start()

    early, late = pl.ds(0, last), pl.ds(1, last)
    for src, kind in (
        (tok.at[early, c], RING), (met.at[early, c], RING_META), (tok.at[:, c], SIDE),
        (met.at[:, c], SIDE_META), (psend, PART), (hid.at[:, 0], HIDDEN), (osend, OUT),
        (ssend.at[late], SUM),
    ):
        remote(src, src, kind, 0, ahead).wait_send()

    @pl.when(c != d)
    def _():
        move_tok.wait_send()
        move_meta.wait_send()
        remote(final, result, GIVE, 0, corner).wait()


def near_layer(tokens, expert_ids, combine, gate, up, down, columns, experts, capacity):
    rows, width = tokens.shape
    held, depth, share = gate.shape
    bf16, f32 = jnp.bfloat16, jnp.float32
    piece = 256 if share % 256 == 0 else 128
    span = width // PIECES
    parts = (held, share // piece, capacity, 2 * piece)
    return pl.pallas_call(
        functools.partial(layer_kernel, columns, experts, capacity),
        out_shape=pltpu.VMEM((rows, width), bf16),
        in_specs=[pl.BlockSpec(memory_space=pltpu.HBM)] * 6,
        out_specs=pl.BlockSpec(memory_space=pltpu.VMEM),
        scratch_shapes=[
            pltpu.VMEM((columns, 2, rows, width), bf16),
            pltpu.VMEM((columns, 2, 2 * experts, 2 * rows), f32),
            pltpu.VMEM((rows, width), bf16),
            pltpu.VMEM((2 * experts, 2 * rows), f32),
            pltpu.VMEM(expert_ids.shape[::-1], jnp.int32),
            pltpu.VMEM(combine.shape[::-1], f32),
            pltpu.VMEM(gate.shape, bf16),
            pltpu.VMEM(up.shape, bf16),
            pltpu.VMEM(down.shape, bf16),
            pltpu.VMEM((held, 2 * capacity, width), bf16),
            pltpu.VMEM((columns, held, 2 * capacity, 2 * rows), bf16),
            pltpu.VMEM((columns, *parts), f32),
            pltpu.VMEM((columns, *parts), bf16),
            pltpu.VMEM((columns, *parts), bf16),
            pltpu.VMEM((columns, 2, held, capacity, share), bf16),
            pltpu.VMEM((2 * rows, held * share), bf16),
            pltpu.VMEM((columns, PIECES, rows, span), f32),
            pltpu.VMEM((columns, PIECES, rows, span), bf16),
            pltpu.VMEM((columns, PIECES, rows, span), bf16),
            pltpu.VMEM((columns, PIECES, rows, span), bf16),
            pltpu.VMEM((columns, PIECES, rows, span), bf16),
            pltpu.VMEM((rows, width), bf16),
            pltpu.SemaphoreType.DMA((11,)),
            pltpu.SemaphoreType.DMA((9, columns)),
            pltpu.SemaphoreType.DMA((2, PIECES)),
            pltpu.SemaphoreType.DMA((2, PIECES)),
            pltpu.SemaphoreType.DMA((2 * held + 4,)),
        ],
        compiler_params=pltpu.CompilerParams(
            collective_id=0, has_side_effects=True, vmem_limit_bytes=60 * 2**20
        ),
    )(tokens, expert_ids.T, combine.T, gate, up, down)


def spread_tokens(tokens, groups, cores, width):
    rows = tokens.shape[0]
    if groups == cores:
        perm = [
            (((d - c) % groups) * cores + d, d * cores + c)
            for d in range(groups)
            for c in range(cores)
        ]
        swapped = lax.ppermute(tokens, ("dp", "etp"), perm)
        along = lax.all_gather(swapped, "expert", axis=0)
        return lax.all_gather(along, "etp", axis=0)
    full = lax.all_gather(tokens, "etp", axis=1, tiled=True)
    mine = lax.all_to_all(
        full.reshape(rows, groups, width), "dp", split_axis=1, concat_axis=0, tiled=False
    )
    mine = mine.reshape(groups, rows, width)
    order = jnp.mod(lax.axis_index("dp") - jnp.arange(groups), groups)
    return lax.all_gather(jnp.take(mine, order, axis=0), "expert", axis=1)


def collect_output(parts, groups, cores, width):
    stacked = jnp.stack(parts)
    if groups == cores:
        summed = lax.psum_scatter(stacked, "etp", scatter_dimension=0, tiled=False)
        summed = lax.psum_scatter(summed, "expert", scatter_dimension=0, tiled=False)
        perm = [
            (d * cores + c, ((d - c) % groups) * cores + d)
            for d in range(groups)
            for c in range(cores)
        ]
        return lax.ppermute(summed, ("dp", "etp"), perm)
    summed = lax.psum_scatter(stacked, "expert", scatter_dimension=1, tiled=False)
    order = jnp.mod(lax.axis_index("dp") - jnp.arange(groups), groups)
    summed = lax.psum(jnp.take(summed, order, axis=0).astype(jnp.float32), "etp")
    back = lax.all_to_all(
        summed.astype(jnp.bfloat16), "dp", split_axis=0, concat_axis=1, tiled=True
    )
    back = back.reshape(back.shape[1] // groups, -1) if back.ndim == 2 else back
    rows = back.shape[-2] // groups
    back = back.reshape(groups, rows, width).transpose(1, 0, 2).reshape(rows, cores, -1)
    return lax.dynamic_index_in_dim(back, lax.axis_index("etp"), 1, keepdims=False)


def shards(tokens, expert_ids, combine, gate_weight, up_weight, down_weight):
    rows, top_count = expert_ids.shape
    held, width, _ = gate_weight.shape
    groups = lax.axis_size("dp")
    columns = lax.axis_size("expert")
    cores = lax.axis_size("etp")
    experts = held * columns
    capacity = min(rows, 3 * rows * top_count // (2 * experts))
    group = lax.axis_index("dp")

    if groups == cores == 2 and columns % 2 == 0 and capacity % 16 == 0 and experts <= 128:
        return near_layer(
            tokens, expert_ids, combine, gate_weight, up_weight, down_weight,
            columns, experts, capacity,
        )
    named = expert_ids[:, :, None] == jnp.arange(experts, dtype=jnp.int32)[None, None, :]
    weight = jnp.sum(jnp.where(named, combine[:, :, None], 0.0), axis=1)
    spread = spread_tokens(tokens, groups, cores, width)
    weight = lax.all_gather(weight.T, ("dp", "expert"), axis=0)
    weight = lax.dynamic_slice_in_dim(weight, lax.axis_index("expert") * held, held, axis=1)
    chosen = (weight > 0).astype(jnp.bfloat16)
    earlier = jnp.triu(jnp.ones((rows, rows), jnp.bfloat16), 1)
    place = jnp.einsum("bet,tu->beu", chosen, earlier, preferred_element_type=jnp.float32)
    slots = jnp.arange(capacity, dtype=jnp.float32)[None, None, :, None]
    hit = (place[:, :, None, :] == slots) & (weight > 0)[:, :, None, :]
    picker = hit.astype(jnp.bfloat16).reshape(groups, columns, held, capacity, rows)
    slot_weight = jnp.sum(jnp.where(hit, weight[:, :, None, :], 0.0), axis=-1)
    slot_weight = slot_weight.reshape(groups, columns, held, capacity)

    def pick(r):
        which = jnp.mod(group - r, groups)
        return lax.dynamic_index_in_dim(picker, which, 0, keepdims=False)

    def gate_up(r):
        packed = jnp.einsum(
            "xest,xtk->exsk", pick(r), spread[r], preferred_element_type=jnp.float32
        )
        packed = packed.astype(jnp.bfloat16).reshape(held, columns * capacity, width)
        found = []
        for e in range(held):
            found.append(
                tuple(
                    jnp.dot(packed[e], w[e], preferred_element_type=jnp.float32)
                    for w in (gate_weight, up_weight)
                )
            )
        return found

    gates = [[] for _ in range(held)]
    ups = [[] for _ in range(held)]
    for r in range(1, groups):
        perm = [(d, (d - r) % groups) for d in range(groups)]
        for e, (g, u) in enumerate(gate_up(r)):
            sent = lax.ppermute(
                jnp.concatenate([g, u], axis=1).astype(jnp.bfloat16), "dp", perm
            )
            half = sent.shape[1] // 2
            gates[e].append(sent[:, :half].astype(jnp.float32))
            ups[e].append(sent[:, half:].astype(jnp.float32))
    own_weight = lax.dynamic_index_in_dim(slot_weight, group, 0, keepdims=False)
    own_weight = own_weight.transpose(1, 0, 2).reshape(held, columns * capacity, 1)
    hidden = [[] for _ in range(groups)]
    for e, (g, u) in enumerate(gate_up(0)):
        g = sum(gates[e], g)
        u = sum(ups[e], u)
        h = (jax.nn.silu(g) * u * own_weight[e]).astype(jnp.bfloat16)
        hidden[0].append(h)
        for r in range(1, groups):
            perm = [(d, (d + r) % groups) for d in range(groups)]
            hidden[r].append(lax.ppermute(h, "dp", perm))

    parts = []
    for r in range(groups):
        h = jnp.stack(hidden[r]).reshape(held, columns, capacity, -1)
        dense = jnp.einsum("xest,exsf->xtef", pick(r), h, preferred_element_type=jnp.float32)
        dense = dense.astype(jnp.bfloat16).reshape(columns * rows, -1)
        out = jnp.dot(
            dense, down_weight.reshape(-1, width), preferred_element_type=jnp.float32
        )
        parts.append(out.astype(jnp.bfloat16).reshape(columns, rows, width))
    return collect_output(parts, groups, cores, width)


def solution(mesh):
    placed = (
        P(("dp", "expert"), "etp"),
        P(("dp", "expert"), None),
        P(("dp", "expert"), None),
        P("expert", "dp", "etp"),
        P("expert", "dp", "etp"),
        P("expert", "etp", "dp"),
    )
    return jax.shard_map(
        shards, mesh=mesh, in_specs=placed, out_specs=P(("dp", "expert"), "etp"), check_vma=False
    )
```

```python
import functools

import jax
import jax.numpy as jnp
from jax import lax
from jax.experimental import pallas as pl
from jax.experimental.pallas import tpu as pltpu
from jax.sharding import PartitionSpec as P

MESH = pl.DeviceIdType.MESH
RING, RING_META, SIDE, SIDE_META, HIDDEN, PART, OUT, SUM, GIVE, MOVE, MOVE_META = range(11)
PIECES = 4


def chunks(size, most):
    step = most if size % most == 0 else 128
    return [slice(n, n + step) for n in range(0, size, step)]


def routing_rows(ids, combine, experts):
    top, rows = ids.shape
    number = lax.broadcasted_iota(jnp.int32, (experts, rows), 0)
    weight = jnp.zeros((experts, rows), jnp.float32)
    chosen = jnp.zeros((experts, rows), jnp.float32)
    for k in range(top):
        same = number == ids[k : k + 1]
        weight = jnp.where(same, combine[k : k + 1], weight)
        chosen = jnp.where(same, 1.0, chosen)
    before = lax.broadcasted_iota(jnp.int32, (rows, rows), 0)
    before = (before < lax.broadcasted_iota(jnp.int32, (rows, rows), 1)).astype(jnp.bfloat16)
    slot = jnp.dot(chosen.astype(jnp.bfloat16), before, preferred_element_type=jnp.float32)
    slot = jnp.where(chosen > 0, slot, -1.0)
    return [jnp.concatenate([a, a], axis=1) for a in (slot, weight)]


def layer_kernel(
    columns, experts, capacity,
    tokens, ids, combine, gate, up, down, result,
    tok, met, stage, mstage, idv, cov, wg, wu, wd, xs, pick, own, psend, precv, hid, dense,
    keep, osend, orecv, ssend, srecv, final, sent, got, ofine, sfine, local,
):
    d, i, c = lax.axis_index("dp"), lax.axis_index("expert"), lax.axis_index("etp")
    held, width, share = wg.shape
    rows = tok.shape[2]
    parts, piece = own.shape[2], own.shape[4] // 2
    span = width // PIECES
    half, last = columns // 2, columns - 1
    odd, line = i % 2, i // 2
    place = (1 - odd) * line + odd * (last - line)

    def at(p):
        p = (p + columns) % columns
        b = p // half
        return (1 - b) * (2 * p) + b * (2 * (last - p) + 1)

    way = 1 - 2 * c
    ahead, behind = (d, at(place + way), c), (d, at(place - way), c)
    side, across, corner = (d, i, 1 - c), (1 - d, i, c), (1 - d, i, 1 - c)

    def copy(src, dst, send, recv, device):
        return pltpu.make_async_remote_copy(
            src_ref=src, dst_ref=dst, send_sem=send, recv_sem=recv,
            device_id=device, device_id_type=MESH,
        )

    def remote(src, dst, kind, r, device):
        return copy(src, dst, sent.at[kind], got.at[kind, r], device)

    def ring_tok(s):
        return remote(tok.at[s, c], tok.at[s + 1, c], RING, s + 1, ahead)

    def ring_meta(s):
        return remote(met.at[s, c], met.at[s + 1, c], RING_META, s + 1, ahead)

    def side_tok(s, g):
        return remote(tok.at[s, g], tok.at[s, g], SIDE, s, side)

    def side_meta(s, g):
        return remote(met.at[s, g], met.at[s, g], SIDE_META, s, side)

    def part_piece(s, e, p):
        return remote(psend.at[s, e, p], precv.at[s, e, p], PART, s, across)

    def part_all(s):
        return remote(psend.at[s], precv.at[s], PART, s, across)

    def hidden_copy(s):
        return remote(hid.at[s, 0], hid.at[s, 1], HIDDEN, s, across)

    def out_piece(s, q, fine):
        sem = ofine.at[(columns - s) % columns, q] if fine else got.at[OUT, s]
        return copy(osend.at[s, q], orecv.at[s, q], sent.at[OUT], sem, side)

    def out_all(s):
        return remote(osend.at[s], orecv.at[s], OUT, s, side)

    def sum_piece(s, after, q, fine):
        sem = sfine.at[(columns - after) % columns, q] if fine else got.at[SUM, after]
        return copy(ssend.at[s, q], srecv.at[after, q], sent.at[SUM], sem, ahead)

    def sum_all(s, after):
        return remote(ssend.at[s], srecv.at[after], SUM, after, ahead)

    def give_piece(q):
        cols = pl.ds(q * span, span)
        return remote(final.at[:, cols], result.at[:, cols], GIVE, 0, corner)

    weights = []
    for e in range(held):
        weights.append(pltpu.make_async_copy(gate.at[e], wg.at[e], local.at[len(weights)]))
        weights.append(pltpu.make_async_copy(up.at[e], wu.at[e], local.at[len(weights)]))
    weights.append(pltpu.make_async_copy(down, wd, local.at[len(weights)]))
    free = len(weights)
    ids_copy = pltpu.make_async_copy(ids, idv, local.at[free])
    combine_copy = pltpu.make_async_copy(combine, cov, local.at[free + 1])
    keep_tok = pltpu.make_async_copy(tokens, tok.at[0, c], local.at[free + 2])
    stage_tok = pltpu.make_async_copy(tokens, stage, local.at[free + 2])
    move_tok = copy(stage, tok.at[0, d], sent.at[MOVE], got.at[RING, 0], corner)
    move_meta = copy(mstage, met.at[0, d], sent.at[MOVE_META], got.at[RING_META, 0], corner)
    got_tok = copy(stage, tok.at[0, c], sent.at[MOVE], got.at[RING, 0], corner)
    got_meta = copy(mstage, met.at[0, c], sent.at[MOVE_META], got.at[RING_META, 0], corner)

    barrier = pltpu.get_barrier_semaphore()
    for device in (ahead, behind, side, across, corner):
        pl.semaphore_signal(barrier, inc=1, device_id=device, device_id_type=MESH)
    ids_copy.start()
    combine_copy.start()
    pl.when(c == d)(lambda: keep_tok.start())
    pl.when(c != d)(lambda: stage_tok.start())
    for w in weights:
        w.start()
    ids_copy.wait()
    combine_copy.wait()
    slot_rows, weight_rows = routing_rows(idv[...], cov[...], experts)
    mstage[:experts] = slot_rows
    mstage[experts:] = weight_rows

    @pl.when(c == d)
    def _():
        met[0, c, :experts] = slot_rows
        met[0, c, experts:] = weight_rows

    pl.semaphore_wait(barrier, 5)

    @pl.when(c != d)
    def _():
        stage_tok.wait()
        move_tok.start()
        move_meta.start()

    lane = lax.broadcasted_iota(jnp.int32, (1, 2 * rows), 1)
    in_first = lane < rows
    kept = (lane < d * rows) | (lane >= (d + 1) * rows)
    slots = lax.broadcasted_iota(jnp.int32, (capacity, 2 * rows), 0).astype(jnp.float32)
    slots_one = lax.broadcasted_iota(jnp.int32, (capacity, rows), 0).astype(jnp.float32)

    def row_of(s, r):
        return jnp.where(in_first, met[s, 0, pl.ds(r, 1), :], met[s, 1, pl.ds(r, 1), :])

    def relay(s):
        @pl.when(s > 0)
        def _():
            ring_tok(s - 1).wait_recv()
            ring_meta(s - 1).wait_recv()

        side_tok(s, c).start()
        side_meta(s, c).start()

        @pl.when(s < last)
        def _():
            ring_tok(s).start()
            ring_meta(s).start()

    def take(s):
        side_tok(s, 1 - c).wait_recv()
        side_meta(s, 1 - c).wait_recv()

    def pack(s, g):
        wide = []
        for e in range(held):
            row = met[s, g, pl.ds(held * i + e, 1), :]
            wide.append(slots_one == row[:, :rows])
        picker = jnp.concatenate(wide).astype(jnp.bfloat16)
        for n in chunks(width, 256):
            packed = jnp.dot(picker, tok[s, g, :, n], preferred_element_type=jnp.float32)
            xs[:, :, n] = packed.astype(jnp.bfloat16).reshape(held, capacity, -1)

    def gate_up(e, p, k):
        w = (wg, wu)[k]
        return jnp.dot(
            xs[e], w[e, :, p * piece : (p + 1) * piece], preferred_element_type=jnp.float32
        )

    def send(s):
        pack(s, d)
        for e in range(held):
            @pl.when(s == 0)
            def _():
                weights[2 * e].wait()
                weights[2 * e + 1].wait()

            for p in range(parts):
                for k in range(2):
                    to = slice(k * piece, (k + 1) * piece)
                    psend[s, e, p, :, to] = gate_up(e, p, k).astype(jnp.bfloat16)
                part_piece(s, e, p).start()

    def keep_part(s):
        pack(s, 1 - d)
        for e in range(held):
            hit = slots == row_of(s, held * i + e)
            pick[s, e, :capacity] = (hit & kept).astype(jnp.bfloat16)
            pick[s, e, capacity:] = (hit & ~kept).astype(jnp.bfloat16)
            for p in range(parts):
                for k in range(2):
                    own[s, e, p, :, k * piece : (k + 1) * piece] = gate_up(e, p, k)

    def middle(s):
        part_all(s).wait_recv()
        for e in range(held):
            hit = (slots == row_of(s, held * i + e)) & kept
            scale = row_of(s, experts + held * i + e)
            scale = jnp.sum(jnp.where(hit, scale, 0.0), axis=1, keepdims=True)
            for p in range(parts):
                g = own[s, e, p, :, :piece] + precv[s, e, p, :, :piece].astype(jnp.float32)
                u = own[s, e, p, :, piece:] + precv[s, e, p, :, piece:].astype(jnp.float32)
                h = g / (1.0 + jnp.exp(-g)) * u * scale
                hid[s, 0, e, :, p * piece : (p + 1) * piece] = h.astype(jnp.bfloat16)

        pl.when(s > 0)(lambda: hidden_copy(s).start())
        pl.when(s == last)(lambda: hidden_copy(0).start())

    def back(s, fine):
        hidden_copy(s).wait_recv()
        for e in range(held):
            for n in chunks(share, 256):
                h = jnp.concatenate([hid[s, 0, e, :, n], hid[s, 1, e, :, n]], axis=0)
                spread = lax.dot_general(
                    pick[s, e], h, (((0,), (0,)), ((), ())), preferred_element_type=jnp.float32
                )
                dense[:, e * share + n.start : e * share + n.stop] = spread.astype(jnp.bfloat16)
        for q in range(PIECES):
            for n in chunks(span, 256):
                v = jnp.dot(
                    dense[...],
                    wd[:, :, q * span + n.start : q * span + n.stop].reshape(held * share, -1),
                    preferred_element_type=jnp.float32,
                )
                low, high = v[:rows], v[rows:]
                keep[s, q, :, n] = jnp.where(c == 0, low, high)
                osend[s, q, :, n] = jnp.where(c == 0, high, low).astype(jnp.bfloat16)
            out_piece(s, q, fine).start()

    def total(s, q):
        return keep[s, q] + orecv[s, q].astype(jnp.float32)

    def collect(s, fine_in, fine_out):
        if not fine_in:
            out_all(s).wait_recv()
            pl.when(s > 1)(lambda: sum_all(s - 1, s).wait_recv())
        for q in range(PIECES):
            if fine_in:
                out_piece(s, q, True).wait_recv()
                sum_piece(s - 1, s, q, True).wait_recv()

            @pl.when(s == 1)
            def _():
                ssend[s, q] = total(s, q).astype(jnp.bfloat16)

            @pl.when(s > 1)
            def _():
                v = total(s, q) + srecv[s, q].astype(jnp.float32)
                ssend[s, q] = v.astype(jnp.bfloat16)

            sum_piece(s, (s + 1) % columns, q, fine_out).start()

    def turn(t, carry):
        @pl.when(c == d)
        def _():
            pl.when(t == 0)(lambda: keep_tok.wait())
            relay(t)

        pl.when(c != d)(lambda: take(t))
        send(t)

        @pl.when(c != d)
        def _():
            @pl.when(t == 0)
            def _():
                got_tok.wait_recv()
                got_meta.wait_recv()

            relay(t)

        @pl.when(t >= 1)
        def _():
            pl.when(c == d)(lambda: take(t - 1))
            keep_part(t - 1)
            pl.when(t >= 2)(lambda: middle(t - 1))

        pl.when(t >= 4)(lambda: collect(t - 3, False, False))

        @pl.when(t == 3)
        def _():
            weights[-1].wait()

        pl.when(t >= 3)(lambda: back(t - 2, False))
        return carry

    lax.fori_loop(0, columns, turn, 0)
    middle(0)
    pl.when(c == d)(lambda: take(last))
    keep_part(last)
    middle(last)
    collect(last - 2, False, True)
    back(last - 1, True)
    collect(last - 1, True, True)
    back(last, True)
    collect(last, True, True)
    back(0, True)
    for q in range(PIECES):
        out_piece(0, q, True).wait_recv()
        sum_piece(last, 0, q, True).wait_recv()
        v = total(0, q) + srecv[0, q].astype(jnp.float32)
        v = v.astype(jnp.bfloat16)

        @pl.when(c == d)
        def _():
            result[:, q * span : (q + 1) * span] = v

        @pl.when(c != d)
        def _():
            final[:, q * span : (q + 1) * span] = v
            give_piece(q).start()

    early, late = pl.ds(0, last), pl.ds(1, last)
    for src, kind in (
        (tok.at[early, c], RING), (met.at[early, c], RING_META), (tok.at[:, c], SIDE),
        (met.at[:, c], SIDE_META), (psend, PART), (hid.at[:, 0], HIDDEN), (osend, OUT),
        (ssend.at[late], SUM),
    ):
        remote(src, src, kind, 0, ahead).wait_send()

    @pl.when(c != d)
    def _():
        move_tok.wait_send()
        move_meta.wait_send()
        remote(final, result, GIVE, 0, corner).wait()


def near_layer(tokens, expert_ids, combine, gate, up, down, columns, experts, capacity):
    rows, width = tokens.shape
    held, depth, share = gate.shape
    bf16, f32 = jnp.bfloat16, jnp.float32
    piece = 256 if share % 256 == 0 else 128
    span = width // PIECES
    parts = (held, share // piece, capacity, 2 * piece)
    return pl.pallas_call(
        functools.partial(layer_kernel, columns, experts, capacity),
        out_shape=pltpu.VMEM((rows, width), bf16),
        in_specs=[pl.BlockSpec(memory_space=pltpu.HBM)] * 6,
        out_specs=pl.BlockSpec(memory_space=pltpu.VMEM),
        scratch_shapes=[
            pltpu.VMEM((columns, 2, rows, width), bf16),
            pltpu.VMEM((columns, 2, 2 * experts, 2 * rows), f32),
            pltpu.VMEM((rows, width), bf16),
            pltpu.VMEM((2 * experts, 2 * rows), f32),
            pltpu.VMEM(expert_ids.shape[::-1], jnp.int32),
            pltpu.VMEM(combine.shape[::-1], f32),
            pltpu.VMEM(gate.shape, bf16),
            pltpu.VMEM(up.shape, bf16),
            pltpu.VMEM(down.shape, bf16),
            pltpu.VMEM((held, capacity, width), bf16),
            pltpu.VMEM((columns, held, 2 * capacity, 2 * rows), bf16),
            pltpu.VMEM((columns, *parts), f32),
            pltpu.VMEM((columns, *parts), bf16),
            pltpu.VMEM((columns, *parts), bf16),
            pltpu.VMEM((columns, 2, held, capacity, share), bf16),
            pltpu.VMEM((2 * rows, held * share), bf16),
            pltpu.VMEM((columns, PIECES, rows, span), f32),
            pltpu.VMEM((columns, PIECES, rows, span), bf16),
            pltpu.VMEM((columns, PIECES, rows, span), bf16),
            pltpu.VMEM((columns, PIECES, rows, span), bf16),
            pltpu.VMEM((columns, PIECES, rows, span), bf16),
            pltpu.VMEM((rows, width), bf16),
            pltpu.SemaphoreType.DMA((11,)),
            pltpu.SemaphoreType.DMA((9, columns)),
            pltpu.SemaphoreType.DMA((3, PIECES)),
            pltpu.SemaphoreType.DMA((3, PIECES)),
            pltpu.SemaphoreType.DMA((2 * held + 4,)),
        ],
        compiler_params=pltpu.CompilerParams(
            collective_id=0, has_side_effects=True, vmem_limit_bytes=60 * 2**20
        ),
    )(tokens, expert_ids.T, combine.T, gate, up, down)


def spread_tokens(tokens, groups, cores, width):
    rows = tokens.shape[0]
    if groups == cores:
        perm = [
            (((d - c) % groups) * cores + d, d * cores + c)
            for d in range(groups)
            for c in range(cores)
        ]
        swapped = lax.ppermute(tokens, ("dp", "etp"), perm)
        along = lax.all_gather(swapped, "expert", axis=0)
        return lax.all_gather(along, "etp", axis=0)
    full = lax.all_gather(tokens, "etp", axis=1, tiled=True)
    mine = lax.all_to_all(
        full.reshape(rows, groups, width), "dp", split_axis=1, concat_axis=0, tiled=False
    )
    mine = mine.reshape(groups, rows, width)
    order = jnp.mod(lax.axis_index("dp") - jnp.arange(groups), groups)
    return lax.all_gather(jnp.take(mine, order, axis=0), "expert", axis=1)


def collect_output(parts, groups, cores, width):
    stacked = jnp.stack(parts)
    if groups == cores:
        summed = lax.psum_scatter(stacked, "etp", scatter_dimension=0, tiled=False)
        summed = lax.psum_scatter(summed, "expert", scatter_dimension=0, tiled=False)
        perm = [
            (d * cores + c, ((d - c) % groups) * cores + d)
            for d in range(groups)
            for c in range(cores)
        ]
        return lax.ppermute(summed, ("dp", "etp"), perm)
    summed = lax.psum_scatter(stacked, "expert", scatter_dimension=1, tiled=False)
    order = jnp.mod(lax.axis_index("dp") - jnp.arange(groups), groups)
    summed = lax.psum(jnp.take(summed, order, axis=0).astype(jnp.float32), "etp")
    back = lax.all_to_all(
        summed.astype(jnp.bfloat16), "dp", split_axis=0, concat_axis=1, tiled=True
    )
    back = back.reshape(back.shape[1] // groups, -1) if back.ndim == 2 else back
    rows = back.shape[-2] // groups
    back = back.reshape(groups, rows, width).transpose(1, 0, 2).reshape(rows, cores, -1)
    return lax.dynamic_index_in_dim(back, lax.axis_index("etp"), 1, keepdims=False)


def shards(tokens, expert_ids, combine, gate_weight, up_weight, down_weight):
    rows, top_count = expert_ids.shape
    held, width, _ = gate_weight.shape
    groups = lax.axis_size("dp")
    columns = lax.axis_size("expert")
    cores = lax.axis_size("etp")
    experts = held * columns
    capacity = min(rows, 3 * rows * top_count // (2 * experts))
    group = lax.axis_index("dp")

    if groups == cores == 2 and columns % 2 == 0 and capacity % 16 == 0 and experts <= 128:
        return near_layer(
            tokens, expert_ids, combine, gate_weight, up_weight, down_weight,
            columns, experts, capacity,
        )
    named = expert_ids[:, :, None] == jnp.arange(experts, dtype=jnp.int32)[None, None, :]
    weight = jnp.sum(jnp.where(named, combine[:, :, None], 0.0), axis=1)
    spread = spread_tokens(tokens, groups, cores, width)
    weight = lax.all_gather(weight.T, ("dp", "expert"), axis=0)
    weight = lax.dynamic_slice_in_dim(weight, lax.axis_index("expert") * held, held, axis=1)
    chosen = (weight > 0).astype(jnp.bfloat16)
    earlier = jnp.triu(jnp.ones((rows, rows), jnp.bfloat16), 1)
    place = jnp.einsum("bet,tu->beu", chosen, earlier, preferred_element_type=jnp.float32)
    slots = jnp.arange(capacity, dtype=jnp.float32)[None, None, :, None]
    hit = (place[:, :, None, :] == slots) & (weight > 0)[:, :, None, :]
    picker = hit.astype(jnp.bfloat16).reshape(groups, columns, held, capacity, rows)
    slot_weight = jnp.sum(jnp.where(hit, weight[:, :, None, :], 0.0), axis=-1)
    slot_weight = slot_weight.reshape(groups, columns, held, capacity)

    def pick(r):
        which = jnp.mod(group - r, groups)
        return lax.dynamic_index_in_dim(picker, which, 0, keepdims=False)

    def gate_up(r):
        packed = jnp.einsum(
            "xest,xtk->exsk", pick(r), spread[r], preferred_element_type=jnp.float32
        )
        packed = packed.astype(jnp.bfloat16).reshape(held, columns * capacity, width)
        found = []
        for e in range(held):
            found.append(
                tuple(
                    jnp.dot(packed[e], w[e], preferred_element_type=jnp.float32)
                    for w in (gate_weight, up_weight)
                )
            )
        return found

    gates = [[] for _ in range(held)]
    ups = [[] for _ in range(held)]
    for r in range(1, groups):
        perm = [(d, (d - r) % groups) for d in range(groups)]
        for e, (g, u) in enumerate(gate_up(r)):
            sent = lax.ppermute(
                jnp.concatenate([g, u], axis=1).astype(jnp.bfloat16), "dp", perm
            )
            half = sent.shape[1] // 2
            gates[e].append(sent[:, :half].astype(jnp.float32))
            ups[e].append(sent[:, half:].astype(jnp.float32))
    own_weight = lax.dynamic_index_in_dim(slot_weight, group, 0, keepdims=False)
    own_weight = own_weight.transpose(1, 0, 2).reshape(held, columns * capacity, 1)
    hidden = [[] for _ in range(groups)]
    for e, (g, u) in enumerate(gate_up(0)):
        g = sum(gates[e], g)
        u = sum(ups[e], u)
        h = (jax.nn.silu(g) * u * own_weight[e]).astype(jnp.bfloat16)
        hidden[0].append(h)
        for r in range(1, groups):
            perm = [(d, (d + r) % groups) for d in range(groups)]
            hidden[r].append(lax.ppermute(h, "dp", perm))

    parts = []
    for r in range(groups):
        h = jnp.stack(hidden[r]).reshape(held, columns, capacity, -1)
        dense = jnp.einsum("xest,exsf->xtef", pick(r), h, preferred_element_type=jnp.float32)
        dense = dense.astype(jnp.bfloat16).reshape(columns * rows, -1)
        out = jnp.dot(
            dense, down_weight.reshape(-1, width), preferred_element_type=jnp.float32
        )
        parts.append(out.astype(jnp.bfloat16).reshape(columns, rows, width))
    return collect_output(parts, groups, cores, width)


def solution(mesh):
    placed = (
        P(("dp", "expert"), "etp"),
        P(("dp", "expert"), None),
        P(("dp", "expert"), None),
        P("expert", "dp", "etp"),
        P("expert", "dp", "etp"),
        P("expert", "etp", "dp"),
    )
    return jax.shard_map(
        shards, mesh=mesh, in_specs=placed, out_specs=P(("dp", "expert"), "etp"), check_vma=False
    )
```

```python
import functools

import jax
import jax.numpy as jnp
from jax import lax
from jax.experimental import pallas as pl
from jax.experimental.pallas import tpu as pltpu
from jax.sharding import PartitionSpec as P

MESH = pl.DeviceIdType.MESH
RING, RING_META, SIDE, SIDE_META, HIDDEN, PART, OUT, SUM, GIVE, MOVE, MOVE_META = range(11)
PIECES = 4


def chunks(size, most):
    step = most if size % most == 0 else 128
    return [slice(n, n + step) for n in range(0, size, step)]


def routing_rows(ids, combine, experts):
    top, rows = ids.shape
    number = lax.broadcasted_iota(jnp.int32, (experts, rows), 0)
    weight = jnp.zeros((experts, rows), jnp.float32)
    chosen = jnp.zeros((experts, rows), jnp.float32)
    for k in range(top):
        same = number == ids[k : k + 1]
        weight = jnp.where(same, combine[k : k + 1], weight)
        chosen = jnp.where(same, 1.0, chosen)
    before = lax.broadcasted_iota(jnp.int32, (rows, rows), 0)
    before = (before < lax.broadcasted_iota(jnp.int32, (rows, rows), 1)).astype(jnp.bfloat16)
    slot = jnp.dot(chosen.astype(jnp.bfloat16), before, preferred_element_type=jnp.float32)
    slot = jnp.where(chosen > 0, slot, -1.0)
    return [jnp.concatenate([a, a], axis=1) for a in (slot, weight)]


def layer_kernel(
    columns, experts, capacity,
    tokens, ids, combine, gate, up, down, result,
    tok, met, stage, mstage, idv, cov, wg, wu, wd, xs, pick, own, psend, precv, hid, dense,
    keep, osend, orecv, ssend, srecv, final, sent, got, ofine, sfine, local,
):
    d, i, c = lax.axis_index("dp"), lax.axis_index("expert"), lax.axis_index("etp")
    held, width, share = wg.shape
    rows = tok.shape[2]
    parts, piece = own.shape[2], own.shape[4] // 2
    span = width // PIECES
    half, last = columns // 2, columns - 1
    odd, line = i % 2, i // 2
    place = (1 - odd) * line + odd * (last - line)

    def at(p):
        p = (p + columns) % columns
        b = p // half
        return (1 - b) * (2 * p) + b * (2 * (last - p) + 1)

    way = 1 - 2 * c
    ahead, behind = (d, at(place + way), c), (d, at(place - way), c)
    side, across, corner = (d, i, 1 - c), (1 - d, i, c), (1 - d, i, 1 - c)

    def copy(src, dst, send, recv, device):
        return pltpu.make_async_remote_copy(
            src_ref=src, dst_ref=dst, send_sem=send, recv_sem=recv,
            device_id=device, device_id_type=MESH,
        )

    def remote(src, dst, kind, r, device):
        return copy(src, dst, sent.at[kind], got.at[kind, r], device)

    def ring_tok(s):
        return remote(tok.at[s, c], tok.at[s + 1, c], RING, s + 1, ahead)

    def ring_meta(s):
        return remote(met.at[s, c], met.at[s + 1, c], RING_META, s + 1, ahead)

    def side_tok(s, g):
        return remote(tok.at[s, g], tok.at[s, g], SIDE, s, side)

    def side_meta(s, g):
        return remote(met.at[s, g], met.at[s, g], SIDE_META, s, side)

    def part_piece(s, e, p):
        return remote(psend.at[s, e, p], precv.at[s, e, p], PART, s, across)

    def part_all(s):
        return remote(psend.at[s], precv.at[s], PART, s, across)

    def hidden_copy(s):
        return remote(hid.at[s, 0], hid.at[s, 1], HIDDEN, s, across)

    def out_piece(s, q, fine):
        sem = ofine.at[(columns - s) % columns, q] if fine else got.at[OUT, s]
        return copy(osend.at[s, q], orecv.at[s, q], sent.at[OUT], sem, side)

    def out_all(s):
        return remote(osend.at[s], orecv.at[s], OUT, s, side)

    def sum_piece(s, after, q, fine):
        sem = sfine.at[(columns - after) % columns, q] if fine else got.at[SUM, after]
        return copy(ssend.at[s, q], srecv.at[after, q], sent.at[SUM], sem, ahead)

    def sum_all(s, after):
        return remote(ssend.at[s], srecv.at[after], SUM, after, ahead)

    def give_piece(q):
        cols = pl.ds(q * span, span)
        return remote(final.at[:, cols], result.at[:, cols], GIVE, 0, corner)

    weights = []
    for e in range(held):
        weights.append(pltpu.make_async_copy(gate.at[e], wg.at[e], local.at[len(weights)]))
        weights.append(pltpu.make_async_copy(up.at[e], wu.at[e], local.at[len(weights)]))
    weights.append(pltpu.make_async_copy(down, wd, local.at[len(weights)]))
    free = len(weights)
    ids_copy = pltpu.make_async_copy(ids, idv, local.at[free])
    combine_copy = pltpu.make_async_copy(combine, cov, local.at[free + 1])
    keep_tok = pltpu.make_async_copy(tokens, tok.at[0, c], local.at[free + 2])
    stage_tok = pltpu.make_async_copy(tokens, stage, local.at[free + 2])
    move_tok = copy(stage, tok.at[0, d], sent.at[MOVE], got.at[RING, 0], corner)
    move_meta = copy(mstage, met.at[0, d], sent.at[MOVE_META], got.at[RING_META, 0], corner)
    got_tok = copy(stage, tok.at[0, c], sent.at[MOVE], got.at[RING, 0], corner)
    got_meta = copy(mstage, met.at[0, c], sent.at[MOVE_META], got.at[RING_META, 0], corner)

    barrier = pltpu.get_barrier_semaphore()
    for device in (ahead, behind, side, across, corner):
        pl.semaphore_signal(barrier, inc=1, device_id=device, device_id_type=MESH)
    ids_copy.start()
    combine_copy.start()
    pl.when(c == d)(lambda: keep_tok.start())
    pl.when(c != d)(lambda: stage_tok.start())
    for w in weights:
        w.start()
    ids_copy.wait()
    combine_copy.wait()
    slot_rows, weight_rows = routing_rows(idv[...], cov[...], experts)
    mstage[:experts] = slot_rows
    mstage[experts:] = weight_rows

    @pl.when(c == d)
    def _():
        met[0, c, :experts] = slot_rows
        met[0, c, experts:] = weight_rows

    pl.semaphore_wait(barrier, 5)

    @pl.when(c != d)
    def _():
        stage_tok.wait()
        move_tok.start()
        move_meta.start()

    lane = lax.broadcasted_iota(jnp.int32, (1, 2 * rows), 1)
    in_first = lane < rows
    kept = (lane < d * rows) | (lane >= (d + 1) * rows)
    slots = lax.broadcasted_iota(jnp.int32, (capacity, 2 * rows), 0).astype(jnp.float32)
    slots_one = lax.broadcasted_iota(jnp.int32, (capacity, rows), 0).astype(jnp.float32)

    def row_of(s, r):
        return jnp.where(in_first, met[s, 0, pl.ds(r, 1), :], met[s, 1, pl.ds(r, 1), :])

    def relay(s):
        @pl.when(s > 0)
        def _():
            ring_tok(s - 1).wait_recv()
            ring_meta(s - 1).wait_recv()

        side_tok(s, c).start()
        side_meta(s, c).start()

        @pl.when(s < last)
        def _():
            ring_tok(s).start()
            ring_meta(s).start()

    def take(s):
        side_tok(s, 1 - c).wait_recv()
        side_meta(s, 1 - c).wait_recv()

    def pack(s, g):
        wide = []
        for e in range(held):
            row = met[s, g, pl.ds(held * i + e, 1), :]
            wide.append(slots_one == row[:, :rows])
        picker = jnp.concatenate(wide).astype(jnp.bfloat16)
        for n in chunks(width, 256):
            packed = jnp.dot(picker, tok[s, g, :, n], preferred_element_type=jnp.float32)
            xs[:, :, n] = packed.astype(jnp.bfloat16).reshape(held, capacity, -1)

    def gate_up(e, p, k):
        w = (wg, wu)[k]
        return jnp.dot(
            xs[e], w[e, :, p * piece : (p + 1) * piece], preferred_element_type=jnp.float32
        )

    def send(s):
        pack(s, d)
        for e in range(held):
            @pl.when(s == 0)
            def _():
                weights[2 * e].wait()
                weights[2 * e + 1].wait()

            for p in range(parts):
                for k in range(2):
                    to = slice(k * piece, (k + 1) * piece)
                    psend[s, e, p, :, to] = gate_up(e, p, k).astype(jnp.bfloat16)
                part_piece(s, e, p).start()

    def keep_part(s):
        pack(s, 1 - d)
        for e in range(held):
            hit = slots == row_of(s, held * i + e)
            pick[s, e, :capacity] = (hit & kept).astype(jnp.bfloat16)
            pick[s, e, capacity:] = (hit & ~kept).astype(jnp.bfloat16)
            for p in range(parts):
                for k in range(2):
                    own[s, e, p, :, k * piece : (k + 1) * piece] = gate_up(e, p, k)

    def middle(s):
        part_all(s).wait_recv()
        for e in range(held):
            hit = (slots == row_of(s, held * i + e)) & kept
            scale = row_of(s, experts + held * i + e)
            scale = jnp.sum(jnp.where(hit, scale, 0.0), axis=1, keepdims=True)
            for p in range(parts):
                g = own[s, e, p, :, :piece] + precv[s, e, p, :, :piece].astype(jnp.float32)
                u = own[s, e, p, :, piece:] + precv[s, e, p, :, piece:].astype(jnp.float32)
                h = g / (1.0 + jnp.exp(-g)) * u * scale
                hid[s, 0, e, :, p * piece : (p + 1) * piece] = h.astype(jnp.bfloat16)

        pl.when(s > 0)(lambda: hidden_copy(s).start())
        pl.when((s == last) & (c == 0))(lambda: hidden_copy(0).start())

    def back(s, fine):
        hidden_copy(s).wait_recv()
        for e in range(held):
            for n in chunks(share, 256):
                h = jnp.concatenate([hid[s, 0, e, :, n], hid[s, 1, e, :, n]], axis=0)
                spread = lax.dot_general(
                    pick[s, e], h, (((0,), (0,)), ((), ())), preferred_element_type=jnp.float32
                )
                dense[:, e * share + n.start : e * share + n.stop] = spread.astype(jnp.bfloat16)
        for q in range(PIECES):
            for n in chunks(span, 256):
                v = jnp.dot(
                    dense[...],
                    wd[:, :, q * span + n.start : q * span + n.stop].reshape(held * share, -1),
                    preferred_element_type=jnp.float32,
                )
                low, high = v[:rows], v[rows:]
                keep[s, q, :, n] = jnp.where(c == 0, low, high)
                osend[s, q, :, n] = jnp.where(c == 0, high, low).astype(jnp.bfloat16)
            out_piece(s, q, fine).start()

    def back_half(s, side_of):
        g = d if side_of else 1 - d
        away = (c + g) % 2
        if side_of:
            hidden_copy(s).wait_recv()
        for e in range(held):
            for n in chunks(share, 256):
                spread = lax.dot_general(
                    pick[s, e, side_of * capacity : (side_of + 1) * capacity],
                    hid[s, side_of, e, :, n], (((0,), (0,)), ((), ())),
                    preferred_element_type=jnp.float32,
                )
                dense[:, e * share + n.start : e * share + n.stop] = spread.astype(jnp.bfloat16)
        for q in range(PIECES):
            for n in chunks(span, 256):
                v = jnp.dot(
                    dense[pl.ds(pl.multiple_of(g * rows, rows), rows), :],
                    wd[:, :, q * span + n.start : q * span + n.stop].reshape(held * share, -1),
                    preferred_element_type=jnp.float32,
                )

                keep[s * (1 - away) + columns * away, q, :, n] = v
                osend[s * away + columns * (1 - away), q, :, n] = v.astype(jnp.bfloat16)

            pl.when(c != g)(lambda: out_piece(s, q, True).start())

    def total(s, q):
        return keep[s, q] + orecv[s, q].astype(jnp.float32)

    def collect(s, fine_in, fine_out):
        if not fine_in:
            out_all(s).wait_recv()
            pl.when(s > 1)(lambda: sum_all(s - 1, s).wait_recv())
        for q in range(PIECES):
            if fine_in:
                out_piece(s, q, True).wait_recv()
                sum_piece(s - 1, s, q, True).wait_recv()

            @pl.when(s == 1)
            def _():
                ssend[s, q] = total(s, q).astype(jnp.bfloat16)

            @pl.when(s > 1)
            def _():
                v = total(s, q) + srecv[s, q].astype(jnp.float32)
                ssend[s, q] = v.astype(jnp.bfloat16)

            sum_piece(s, (s + 1) % columns, q, fine_out).start()

    def turn(t, carry):
        @pl.when(c == d)
        def _():
            pl.when(t == 0)(lambda: keep_tok.wait())
            relay(t)

        pl.when(c != d)(lambda: take(t))
        send(t)
        pl.when(t >= 4)(lambda: collect(t - 3, False, False))

        @pl.when(c != d)
        def _():
            @pl.when(t == 0)
            def _():
                got_tok.wait_recv()
                got_meta.wait_recv()

            relay(t)

        @pl.when(t >= 1)
        def _():
            pl.when(c == d)(lambda: take(t - 1))
            keep_part(t - 1)
            pl.when(t >= 2)(lambda: middle(t - 1))

        @pl.when(t == 3)
        def _():
            weights[-1].wait()

        pl.when(t >= 3)(lambda: back(t - 2, False))
        return carry

    lax.fori_loop(0, columns, turn, 0)
    middle(0)
    pl.when(c == d)(lambda: take(last))
    keep_part(last)
    back_half(last - 1, 0)
    collect(last - 2, False, True)
    back_half(0, 0)
    middle(last)
    back_half(last, 0)
    pl.when(c != d)(lambda: collect(last - 1, True, True))
    back_half(last - 1, 1)
    pl.when(c == 1)(lambda: hidden_copy(0).start())
    pl.when(c == d)(lambda: collect(last - 1, True, True))
    pl.when(c != d)(lambda: collect(last, True, True))
    back_half(last, 1)

    def finish(q):
        out_piece(0, q, True).wait_recv()
        sum_piece(last, 0, q, True).wait_recv()
        return (total(0, q) + srecv[0, q].astype(jnp.float32)).astype(jnp.bfloat16)

    @pl.when(c == d)
    def _():
        collect(last, True, True)

    @pl.when(c != d)
    def _():
        for q in range(PIECES):
            final[:, q * span : (q + 1) * span] = finish(q)
            give_piece(q).start()

    back_half(0, 1)

    @pl.when(c == d)
    def _():
        for q in range(PIECES):
            result[:, q * span : (q + 1) * span] = finish(q)

    early, late = pl.ds(0, last), pl.ds(1, last)
    for src, kind in (
        (tok.at[early, c], RING), (met.at[early, c], RING_META), (tok.at[:, c], SIDE),
        (met.at[:, c], SIDE_META), (psend, PART), (hid.at[:, 0], HIDDEN), (osend.at[pl.ds(0, columns)], OUT),
        (ssend.at[late], SUM),
    ):
        remote(src, src, kind, 0, ahead).wait_send()

    @pl.when(c != d)
    def _():
        move_tok.wait_send()
        move_meta.wait_send()
        remote(final, result, GIVE, 0, corner).wait()


def near_layer(tokens, expert_ids, combine, gate, up, down, columns, experts, capacity):
    rows, width = tokens.shape
    held, depth, share = gate.shape
    bf16, f32 = jnp.bfloat16, jnp.float32
    piece = 256 if share % 256 == 0 else 128
    span = width // PIECES
    parts = (held, share // piece, capacity, 2 * piece)
    return pl.pallas_call(
        functools.partial(layer_kernel, columns, experts, capacity),
        out_shape=pltpu.VMEM((rows, width), bf16),
        in_specs=[pl.BlockSpec(memory_space=pltpu.HBM)] * 6,
        out_specs=pl.BlockSpec(memory_space=pltpu.VMEM),
        scratch_shapes=[
            pltpu.VMEM((columns, 2, rows, width), bf16),
            pltpu.VMEM((columns, 2, 2 * experts, 2 * rows), f32),
            pltpu.VMEM((rows, width), bf16),
            pltpu.VMEM((2 * experts, 2 * rows), f32),
            pltpu.VMEM(expert_ids.shape[::-1], jnp.int32),
            pltpu.VMEM(combine.shape[::-1], f32),
            pltpu.VMEM(gate.shape, bf16),
            pltpu.VMEM(up.shape, bf16),
            pltpu.VMEM(down.shape, bf16),
            pltpu.VMEM((held, capacity, width), bf16),
            pltpu.VMEM((columns, held, 2 * capacity, 2 * rows), bf16),
            pltpu.VMEM((columns, *parts), f32),
            pltpu.VMEM((columns, *parts), bf16),
            pltpu.VMEM((columns, *parts), bf16),
            pltpu.VMEM((columns, 2, held, capacity, share), bf16),
            pltpu.VMEM((2 * rows, held * share), bf16),
            pltpu.VMEM((columns + 1, PIECES, rows, span), f32),
            pltpu.VMEM((columns + 1, PIECES, rows, span), bf16),
            pltpu.VMEM((columns, PIECES, rows, span), bf16),
            pltpu.VMEM((columns, PIECES, rows, span), bf16),
            pltpu.VMEM((columns, PIECES, rows, span), bf16),
            pltpu.VMEM((rows, width), bf16),
            pltpu.SemaphoreType.DMA((11,)),
            pltpu.SemaphoreType.DMA((9, columns)),
            pltpu.SemaphoreType.DMA((3, PIECES)),
            pltpu.SemaphoreType.DMA((3, PIECES)),
            pltpu.SemaphoreType.DMA((2 * held + 4,)),
        ],
        compiler_params=pltpu.CompilerParams(
            collective_id=0, has_side_effects=True, vmem_limit_bytes=60 * 2**20
        ),
    )(tokens, expert_ids.T, combine.T, gate, up, down)


def spread_tokens(tokens, groups, cores, width):
    rows = tokens.shape[0]
    if groups == cores:
        perm = [
            (((d - c) % groups) * cores + d, d * cores + c)
            for d in range(groups)
            for c in range(cores)
        ]
        swapped = lax.ppermute(tokens, ("dp", "etp"), perm)
        along = lax.all_gather(swapped, "expert", axis=0)
        return lax.all_gather(along, "etp", axis=0)
    full = lax.all_gather(tokens, "etp", axis=1, tiled=True)
    mine = lax.all_to_all(
        full.reshape(rows, groups, width), "dp", split_axis=1, concat_axis=0, tiled=False
    )
    mine = mine.reshape(groups, rows, width)
    order = jnp.mod(lax.axis_index("dp") - jnp.arange(groups), groups)
    return lax.all_gather(jnp.take(mine, order, axis=0), "expert", axis=1)


def collect_output(parts, groups, cores, width):
    stacked = jnp.stack(parts)
    if groups == cores:
        summed = lax.psum_scatter(stacked, "etp", scatter_dimension=0, tiled=False)
        summed = lax.psum_scatter(summed, "expert", scatter_dimension=0, tiled=False)
        perm = [
            (d * cores + c, ((d - c) % groups) * cores + d)
            for d in range(groups)
            for c in range(cores)
        ]
        return lax.ppermute(summed, ("dp", "etp"), perm)
    summed = lax.psum_scatter(stacked, "expert", scatter_dimension=1, tiled=False)
    order = jnp.mod(lax.axis_index("dp") - jnp.arange(groups), groups)
    summed = lax.psum(jnp.take(summed, order, axis=0).astype(jnp.float32), "etp")
    back = lax.all_to_all(
        summed.astype(jnp.bfloat16), "dp", split_axis=0, concat_axis=1, tiled=True
    )
    back = back.reshape(back.shape[1] // groups, -1) if back.ndim == 2 else back
    rows = back.shape[-2] // groups
    back = back.reshape(groups, rows, width).transpose(1, 0, 2).reshape(rows, cores, -1)
    return lax.dynamic_index_in_dim(back, lax.axis_index("etp"), 1, keepdims=False)


def shards(tokens, expert_ids, combine, gate_weight, up_weight, down_weight):
    rows, top_count = expert_ids.shape
    held, width, _ = gate_weight.shape
    groups = lax.axis_size("dp")
    columns = lax.axis_size("expert")
    cores = lax.axis_size("etp")
    experts = held * columns
    capacity = min(rows, 3 * rows * top_count // (2 * experts))
    group = lax.axis_index("dp")

    if groups == cores == 2 and columns % 2 == 0 and capacity % 16 == 0 and experts <= 128:
        return near_layer(
            tokens, expert_ids, combine, gate_weight, up_weight, down_weight,
            columns, experts, capacity,
        )
    named = expert_ids[:, :, None] == jnp.arange(experts, dtype=jnp.int32)[None, None, :]
    weight = jnp.sum(jnp.where(named, combine[:, :, None], 0.0), axis=1)
    spread = spread_tokens(tokens, groups, cores, width)
    weight = lax.all_gather(weight.T, ("dp", "expert"), axis=0)
    weight = lax.dynamic_slice_in_dim(weight, lax.axis_index("expert") * held, held, axis=1)
    chosen = (weight > 0).astype(jnp.bfloat16)
    earlier = jnp.triu(jnp.ones((rows, rows), jnp.bfloat16), 1)
    place = jnp.einsum("bet,tu->beu", chosen, earlier, preferred_element_type=jnp.float32)
    slots = jnp.arange(capacity, dtype=jnp.float32)[None, None, :, None]
    hit = (place[:, :, None, :] == slots) & (weight > 0)[:, :, None, :]
    picker = hit.astype(jnp.bfloat16).reshape(groups, columns, held, capacity, rows)
    slot_weight = jnp.sum(jnp.where(hit, weight[:, :, None, :], 0.0), axis=-1)
    slot_weight = slot_weight.reshape(groups, columns, held, capacity)

    def pick(r):
        which = jnp.mod(group - r, groups)
        return lax.dynamic_index_in_dim(picker, which, 0, keepdims=False)

    def gate_up(r):
        packed = jnp.einsum(
            "xest,xtk->exsk", pick(r), spread[r], preferred_element_type=jnp.float32
        )
        packed = packed.astype(jnp.bfloat16).reshape(held, columns * capacity, width)
        found = []
        for e in range(held):
            found.append(
                tuple(
                    jnp.dot(packed[e], w[e], preferred_element_type=jnp.float32)
                    for w in (gate_weight, up_weight)
                )
            )
        return found

    gates = [[] for _ in range(held)]
    ups = [[] for _ in range(held)]
    for r in range(1, groups):
        perm = [(d, (d - r) % groups) for d in range(groups)]
        for e, (g, u) in enumerate(gate_up(r)):
            sent = lax.ppermute(
                jnp.concatenate([g, u], axis=1).astype(jnp.bfloat16), "dp", perm
            )
            half = sent.shape[1] // 2
            gates[e].append(sent[:, :half].astype(jnp.float32))
            ups[e].append(sent[:, half:].astype(jnp.float32))
    own_weight = lax.dynamic_index_in_dim(slot_weight, group, 0, keepdims=False)
    own_weight = own_weight.transpose(1, 0, 2).reshape(held, columns * capacity, 1)
    hidden = [[] for _ in range(groups)]
    for e, (g, u) in enumerate(gate_up(0)):
        g = sum(gates[e], g)
        u = sum(ups[e], u)
        h = (jax.nn.silu(g) * u * own_weight[e]).astype(jnp.bfloat16)
        hidden[0].append(h)
        for r in range(1, groups):
            perm = [(d, (d + r) % groups) for d in range(groups)]
            hidden[r].append(lax.ppermute(h, "dp", perm))

    parts = []
    for r in range(groups):
        h = jnp.stack(hidden[r]).reshape(held, columns, capacity, -1)
        dense = jnp.einsum("xest,exsf->xtef", pick(r), h, preferred_element_type=jnp.float32)
        dense = dense.astype(jnp.bfloat16).reshape(columns * rows, -1)
        out = jnp.dot(
            dense, down_weight.reshape(-1, width), preferred_element_type=jnp.float32
        )
        parts.append(out.astype(jnp.bfloat16).reshape(columns, rows, width))
    return collect_output(parts, groups, cores, width)


def solution(mesh):
    placed = (
        P(("dp", "expert"), "etp"),
        P(("dp", "expert"), None),
        P(("dp", "expert"), None),
        P("expert", "dp", "etp"),
        P("expert", "dp", "etp"),
        P("expert", "etp", "dp"),
    )
    return jax.shard_map(
        shards, mesh=mesh, in_specs=placed, out_specs=P(("dp", "expert"), "etp"), check_vma=False
    )
```
